32 devices in a mesh: dp: 2 (over x), sp2: 4 (over z), sp: 4 (over y, core).
Axes of the slice: x: 2, y: 2, z: 4, core: 2. Of those that a mesh axis runs over, the one named last changes fastest.
Arguments:
- x: bfloat16 [16, 16, 128, 1280], P('dp', 'sp', 'sp2'), parts along dimension 0
- time_emb: bfloat16 [16, 1280], P('dp'), parts along dimension 0
- gn_scale: bfloat16 [5, 1280], replicated
- gn_shift: bfloat16 [5, 1280], replicated
- conv_w: bfloat16 [4, 3, 3, 1280, 1280], replicated
- time_w: bfloat16 [2, 1280, 1280], replicated
- w_qkv: bfloat16 [3, 1280, 20, 64], replicated
- w_out: bfloat16 [20, 64, 1280], replicated
Outputs:
- output: bfloat16 [16, 16, 128, 1280], P('dp', 'sp', 'sp2'), parts along dimension 0
There are 2 independent parts. The reference program is written for one: setup_inputs(seed, part) draws one part's arguments, and reference() takes and returns one part's arrays. A program takes and returns all parts, laid end to end along the dimension named above; an argument that names none is the same for every part.
All inputs are finite; a program needn't handle non-finite values.
Results may differ from the reference program's by a relative error of at most 0.00966543.
Values are sent between devices in bfloat16 or wider.
A program may use at most 1 GiB of HBM per device.

```python
import jax
import jax.numpy as jnp
from jax import lax

IMAGES = 8
LAT_ROWS = 16
LAT_COLS = 128
CHANNELS = 1280
NUM_HEADS = 20
TEMB_DIM = 1280
QUERY_BLOCK = 128
GROUPS = 32
NORM_EPS = 1e-5


def setup_inputs(seed: int = 0, part: int = 0) -> dict:
    base = jax.random.key(seed)
    part_keys = jax.random.split(jax.random.fold_in(base, part), 4)
    shared = jax.random.split(base, 6)
    head_dim = CHANNELS // NUM_HEADS
    ramp_rows = (jnp.arange(LAT_ROWS, dtype=jnp.float32) + 0.5) / LAT_ROWS * 2.0 - 1.0
    ramp_cols = (jnp.arange(LAT_COLS, dtype=jnp.float32) + 0.5) / LAT_COLS * 2.0 - 1.0
    slope_rows = jax.random.normal(part_keys[0], (IMAGES, 1, 1, CHANNELS), jnp.float32)
    slope_cols = jax.random.normal(part_keys[1], (IMAGES, 1, 1, CHANNELS), jnp.float32)
    noise = jax.random.normal(part_keys[2], (IMAGES, LAT_ROWS, LAT_COLS, CHANNELS), jnp.float32)
    latent = noise + 1.2 * (slope_rows * ramp_rows[None, :, None, None] + slope_cols * ramp_cols[None, None, :, None])
    time_emb = jax.random.normal(part_keys[3], (IMAGES, TEMB_DIM), jnp.float32)
    gn_scale = 1.0 + 0.3 * jax.random.normal(shared[0], (5, CHANNELS), jnp.float32)
    gn_shift = 0.5 * jax.random.normal(shared[1], (5, CHANNELS), jnp.float32)
    conv_w = jax.random.normal(shared[2], (4, 3, 3, CHANNELS, CHANNELS), jnp.float32) * (9 * CHANNELS) ** -0.5
    time_w = jax.random.normal(shared[3], (2, TEMB_DIM, CHANNELS), jnp.float32) * TEMB_DIM ** -0.5
    qkv_gain = jnp.array([1.5, 1.5, 1.0], jnp.float32)[:, None, None, None]
    w_qkv = jax.random.normal(shared[4], (3, CHANNELS, NUM_HEADS, head_dim), jnp.float32) * CHANNELS ** -0.5 * qkv_gain
    w_out = jax.random.normal(shared[5], (NUM_HEADS, head_dim, CHANNELS), jnp.float32) * CHANNELS ** -0.5
    return {
        "x": latent.astype(jnp.bfloat16),
        "time_emb": time_emb.astype(jnp.bfloat16),
        "gn_scale": gn_scale.astype(jnp.bfloat16),
        "gn_shift": gn_shift.astype(jnp.bfloat16),
        "conv_w": conv_w.astype(jnp.bfloat16),
        "time_w": time_w.astype(jnp.bfloat16),
        "w_qkv": w_qkv.astype(jnp.bfloat16),
        "w_out": w_out.astype(jnp.bfloat16),
    }


def group_norm(latent, scale, shift):
    batch, height, width, channels = latent.shape
    grouped = latent.astype(jnp.float32).reshape(batch, height, width, GROUPS, channels // GROUPS)
    mean = jnp.mean(grouped, axis=(1, 2, 4), keepdims=True)
    mean_sq = jnp.mean(grouped * grouped, axis=(1, 2, 4), keepdims=True)
    normed = (grouped - mean) * lax.rsqrt(mean_sq - mean * mean + NORM_EPS)
    return normed.reshape(latent.shape) * scale.astype(jnp.float32) + shift.astype(jnp.float32)


def conv3x3(latent, kernel):
    return lax.conv_general_dilated(latent.astype(jnp.float32), kernel.astype(jnp.float32), (1, 1), "SAME", dimension_numbers=("NHWC", "HWIO", "NHWC"))


def res_block(latent, time_vec, gn_scale, gn_shift, conv_w, norm_idx, conv_idx):
    first = jax.nn.silu(group_norm(latent, gn_scale[norm_idx], gn_shift[norm_idx])).astype(jnp.bfloat16)
    hidden = (conv3x3(first, conv_w[conv_idx]) + time_vec[:, None, None, :]).astype(jnp.bfloat16)
    second = jax.nn.silu(group_norm(hidden, gn_scale[norm_idx + 1], gn_shift[norm_idx + 1])).astype(jnp.bfloat16)
    return (latent.astype(jnp.float32) + conv3x3(second, conv_w[conv_idx + 1])).astype(jnp.bfloat16)


def attention_block(latent, scale, shift, w_qkv, w_out):
    batch = latent.shape[0]
    tokens = LAT_ROWS * LAT_COLS
    head_dim = CHANNELS // NUM_HEADS
    normed = group_norm(latent, scale, shift).astype(jnp.bfloat16).reshape(batch, tokens, CHANNELS)
    projected = jnp.einsum("bnc,schd->sbnhd", normed.astype(jnp.float32), w_qkv.astype(jnp.float32)).astype(jnp.bfloat16)
    keys = projected[1].astype(jnp.float32)
    values = projected[2].astype(jnp.float32)
    w_out32 = w_out.astype(jnp.float32)
    query_blocks = jnp.moveaxis(projected[0].reshape(batch, tokens // QUERY_BLOCK, QUERY_BLOCK, NUM_HEADS, head_dim), 1, 0)

    def one_block(q_blk):
        logits = jnp.einsum("bqhd,bkhd->bhqk", q_blk.astype(jnp.float32), keys) * head_dim ** -0.5
        weights = jnp.exp(logits - jnp.max(logits, axis=-1, keepdims=True))
        weight_sum = jnp.sum(weights, axis=-1)
        attended = jnp.einsum("bhqk,bkhd->bhqd", weights.astype(jnp.bfloat16).astype(jnp.float32), values) / weight_sum[..., None]
        return jnp.einsum("bhqd,hdc->bqc", attended.astype(jnp.bfloat16).astype(jnp.float32), w_out32)

    out = jnp.moveaxis(lax.map(one_block, query_blocks), 0, 1).reshape(latent.shape)
    return (latent.astype(jnp.float32) + out).astype(jnp.bfloat16)


def reference(x, time_emb, gn_scale, gn_shift, conv_w, time_w, w_qkv, w_out):
    time_act = jax.nn.silu(time_emb.astype(jnp.float32)).astype(jnp.bfloat16)
    time_first = jnp.dot(time_act, time_w[0], preferred_element_type=jnp.float32)
    time_second = jnp.dot(time_act, time_w[1], preferred_element_type=jnp.float32)
    first = res_block(x, time_first, gn_scale, gn_shift, conv_w, 0, 0)
    middle = attention_block(first, gn_scale[2], gn_shift[2], w_qkv, w_out)
    return res_block(middle, time_second, gn_scale, gn_shift, conv_w, 3, 2)
```

```python
import functools

import jax
import jax.numpy as jnp
from jax import lax
from jax.experimental import pallas as pl
from jax.experimental.pallas import tpu as pltpu
from jax.sharding import PartitionSpec as P

GROUPS = 32
NORM_EPS = 1e-5
MESH = pl.DeviceIdType.MESH
SP, SP2 = "sp", "sp2"


def place(sp, cores=2):
    return sp // cores, lax.rem(sp, cores)


def to_images_kernel(x_ref, out_ref, stage, send_sem, recv_sem, self_sem):
    images, rows, cols, _ = x_ref.shape
    sp, z = lax.axis_index(SP), lax.axis_index(SP2)
    y, core = place(sp)
    mine = y * 4 + z
    to_core = z // 2
    own = to_core == core
    barrier = pltpu.get_barrier_semaphore()
    for s in range(8):
        src_sp, src_z = s // 2, 2 * core + s % 2

        @pl.when(jnp.logical_not((src_sp == sp) & (src_z == z)))
        def _():
            pl.semaphore_signal(barrier, inc=1, device_id={SP: src_sp, SP2: src_z}, device_id_type=MESH)

    pl.semaphore_wait(barrier, 8 - own.astype(jnp.int32))

    def piece(src_sp, src_z):
        return out_ref.at[pl.ds(src_sp * rows, rows), pl.ds(lax.rem(src_z, 2) * cols, cols), :]

    def send(i):
        return pltpu.make_async_remote_copy(
            src_ref=x_ref.at[i], dst_ref=piece(sp, z), send_sem=send_sem.at[i], recv_sem=recv_sem.at[sp * 2 + lax.rem(z, 2)],
            device_id={SP: (i // 4) * 2 + to_core, SP2: i % 4}, device_id_type=MESH)

    def is_self(i):
        return own & (mine == i)

    for i in range(images):
        @pl.when(jnp.logical_not(is_self(i)))
        def _():
            send(i).start()

    @pl.when(own)
    def _():
        load = pltpu.make_async_copy(x_ref.at[mine], stage, self_sem)
        load.start()
        load.wait()
        store = pltpu.make_async_copy(stage, piece(sp, z), self_sem)
        store.start()
        store.wait()

    for s in range(8):
        src_sp, src_z = s // 2, 2 * core + s % 2

        @pl.when(jnp.logical_not((src_sp == sp) & (src_z == z)))
        def _():
            pltpu.make_async_remote_copy(
                src_ref=x_ref.at[0], dst_ref=piece(src_sp, src_z), send_sem=send_sem.at[0], recv_sem=recv_sem.at[s],
                device_id={SP: src_sp, SP2: src_z}, device_id_type=MESH).wait_recv()

    for i in range(images):
        @pl.when(jnp.logical_not(is_self(i)))
        def _():
            send(i).wait_send()


def to_images(x):
    images, rows, cols, channels = x.shape
    return pl.pallas_call(
        to_images_kernel,
        out_shape=jax.ShapeDtypeStruct((4 * rows, 2 * cols, channels), x.dtype),
        in_specs=[pl.BlockSpec(memory_space=pl.ANY)],
        out_specs=pl.BlockSpec(memory_space=pl.ANY),
        scratch_shapes=[pltpu.VMEM((rows, cols, channels), x.dtype), pltpu.SemaphoreType.DMA((8,)), pltpu.SemaphoreType.DMA((8,)), pltpu.SemaphoreType.DMA],
        compiler_params=pltpu.CompilerParams(collective_id=0, has_side_effects=True),
        name="to_images",
    )(x)


def to_tiles_kernel(h_ref, out_ref, stage, send_sem, recv_sem, self_sem):
    images, rows, cols, _ = out_ref.shape
    sp, z = lax.axis_index(SP), lax.axis_index(SP2)
    y, core = place(sp)
    mine = y * 4 + z
    from_core = z // 2
    own = from_core == core
    barrier = pltpu.get_barrier_semaphore()
    for i in range(images):
        @pl.when(jnp.logical_not(own & (mine == i)))
        def _():
            pl.semaphore_signal(barrier, inc=1, device_id={SP: (i // 4) * 2 + from_core, SP2: i % 4}, device_id_type=MESH)

    pl.semaphore_wait(barrier, 8 - own.astype(jnp.int32))

    def piece(dst_sp, dst_z):
        return h_ref.at[pl.ds(dst_sp * rows, rows), pl.ds(lax.rem(dst_z, 2) * cols, cols), :]

    def send(s):
        dst_sp, dst_z = s // 2, 2 * core + s % 2
        return pltpu.make_async_remote_copy(
            src_ref=piece(dst_sp, dst_z), dst_ref=out_ref.at[mine], send_sem=send_sem.at[s], recv_sem=recv_sem.at[mine],
            device_id={SP: dst_sp, SP2: dst_z}, device_id_type=MESH)

    def is_self(s):
        return (s // 2 == sp) & (2 * core + s % 2 == z)

    for s in range(8):
        @pl.when(jnp.logical_not(is_self(s)))
        def _():
            send(s).start()

    @pl.when(own)
    def _():
        load = pltpu.make_async_copy(piece(sp, z), stage, self_sem)
        load.start()
        load.wait()
        store = pltpu.make_async_copy(stage, out_ref.at[mine], self_sem)
        store.start()
        store.wait()

    for i in range(images):
        @pl.when(jnp.logical_not(own & (mine == i)))
        def _():
            pltpu.make_async_remote_copy(
                src_ref=piece(0, 0), dst_ref=out_ref.at[i], send_sem=send_sem.at[0], recv_sem=recv_sem.at[i],
                device_id={SP: (i // 4) * 2 + from_core, SP2: i % 4}, device_id_type=MESH).wait_recv()

    for s in range(8):
        @pl.when(jnp.logical_not(is_self(s)))
        def _():
            send(s).wait_send()


def to_tiles(h):
    rows, cols, channels = h.shape[0] // 4, h.shape[1] // 2, h.shape[2]
    return pl.pallas_call(
        to_tiles_kernel,
        out_shape=jax.ShapeDtypeStruct((8, rows, cols, channels), h.dtype),
        in_specs=[pl.BlockSpec(memory_space=pl.ANY)],
        out_specs=pl.BlockSpec(memory_space=pl.ANY),
        scratch_shapes=[pltpu.VMEM((rows, cols, channels), h.dtype), pltpu.SemaphoreType.DMA((8,)), pltpu.SemaphoreType.DMA((8,)), pltpu.SemaphoreType.DMA],
        compiler_params=pltpu.CompilerParams(collective_id=1, has_side_effects=True),
        name="to_tiles",
    )(h)


def swap_cores(value):
    return lax.ppermute(value, SP, [(0, 1), (1, 0), (2, 3), (3, 2)])


def silu(v):
    return v / (1.0 + jnp.exp(-v))

def conv_kernel(steps, mb, residual, core_ref, h_ref, other_ref, norm_ref, w_ref, add_ref, out_ref, sums_ref, act, acc):
    rows, cols, channels = h_ref.shape
    n, t = pl.program_id(0), pl.program_id(1)
    taps = 9 // steps

    @pl.when((n == 0) & (t == 0))
    def _():
        core = core_ref[0]
        mean, mult, shift = norm_ref[0:1, :], norm_ref[1:2, :], norm_ref[2:3, :]

        def activate(v):
            return silu((v.astype(jnp.float32) - mean) * mult + shift)

        zeros = jnp.zeros((cols, channels), jnp.bfloat16)
        for dx in range(3):
            act[dx, 0] = zeros
            act[dx, rows + 1] = zeros
        line = lax.broadcasted_iota(jnp.int32, (cols, channels), 0)

        def one_row(r, carry):
            u = activate(h_ref[r])
            edge = activate(other_ref[r])
            left = jnp.where(core == 1, edge, 0.0)
            right = jnp.where(core == 0, edge, 0.0)
            act[1, r + 1] = u.astype(jnp.bfloat16)
            act[0, r + 1] = jnp.where(line == 0, left, pltpu.roll(u, 1, 0)).astype(jnp.bfloat16)
            act[2, r + 1] = jnp.where(line == cols - 1, right, pltpu.roll(u, cols - 1, 0)).astype(jnp.bfloat16)
            return carry

        lax.fori_loop(0, rows, one_row, 0)

    mrows = mb // cols
    width = w_ref.shape[-1]

    def block(m, carry):
        total = None
        for k in range(taps):
            if steps == 9:
                dy, dx = t // 3, lax.rem(t, 3)
            elif steps == 3:
                dy, dx = t, k
            else:
                dy, dx = k // 3, k % 3
            lhs = act[dx, pl.ds(m * mrows + dy, mrows)].reshape(mb, channels)
            part = jnp.dot(lhs, w_ref[0, k] if steps != 1 else w_ref[dy, dx], preferred_element_type=jnp.float32)
            total = part if total is None else total + part
        rowsl = pl.ds(m * mb, mb)
        if steps > 1:
            @pl.when(t == 0)
            def _():
                acc[rowsl, :] = total
            @pl.when((t > 0) & (t < steps - 1))
            def _():
                acc[rowsl, :] += total
        def finish():
            full = acc[rowsl, :] + total if steps > 1 else total
            if residual:
                full = full + add_ref[pl.ds(m * mrows, mrows)].reshape(mb, width).astype(jnp.float32)
            else:
                full = full + add_ref[...]
            half = full.astype(jnp.bfloat16)
            out_ref[pl.ds(m * mrows, mrows)] = half.reshape(mrows, cols, width)
            kept = half.astype(jnp.float32)
            s = jnp.concatenate([jnp.sum(kept, axis=0, keepdims=True), jnp.sum(kept * kept, axis=0, keepdims=True)], axis=0)
            @pl.when(m == 0)
            def _():
                sums_ref[...] = s
            @pl.when(m > 0)
            def _():
                sums_ref[...] += s
        if steps > 1:
            pl.when(t == steps - 1)(finish)
        else:
            finish()
        return carry

    lax.fori_loop(0, rows * cols // mb, block, 0)

def conv(core, h, other, norm, w, j, add, nb=256, steps=1, mb=1024):
    rows, cols, channels = h.shape
    residual = add.ndim == 3
    outw = w.shape[-1]
    whole = lambda *s: pl.BlockSpec(s, lambda n, t: (0,) * len(s))
    if steps == 9:
        wspec = pl.BlockSpec((None, 1, 1, channels, nb), lambda n, t: (j, t // 3, t % 3, 0, n))
    elif steps == 3:
        wspec = pl.BlockSpec((None, 1, 3, channels, nb), lambda n, t: (j, t, 0, 0, n))
    else:
        wspec = pl.BlockSpec((None, 3, 3, channels, nb), lambda n, t: (j, 0, 0, 0, n))
    addspec = pl.BlockSpec((rows, cols, nb), lambda n, t: (0, 0, n)) if residual else pl.BlockSpec((1, nb), lambda n, t: (0, n))
    return pl.pallas_call(
        functools.partial(conv_kernel, steps, mb, residual),
        grid=(outw // nb, steps),
        in_specs=[pl.BlockSpec(memory_space=pltpu.SMEM), whole(rows, cols, channels), whole(rows, 1, channels), whole(3, channels), wspec, addspec],
        out_specs=[pl.BlockSpec((rows, cols, nb), lambda n, t: (0, 0, n)), pl.BlockSpec((2, nb), lambda n, t: (0, n))],
        out_shape=[jax.ShapeDtypeStruct((rows, cols, outw), jnp.bfloat16), jax.ShapeDtypeStruct((2, outw), jnp.float32)],
        scratch_shapes=[pltpu.VMEM((3, rows + 2, cols, channels), jnp.bfloat16), pltpu.VMEM((rows * cols if steps > 1 else 8, nb), jnp.float32)],
        compiler_params=pltpu.CompilerParams(vmem_limit_bytes=62 * 1024 * 1024),
        name="conv",
    )(core, h, other, norm, w, add)


NT = (((1,), (1,)), ((), ()))

def attend_kernel(q_ref, k0_ref, k1_ref, v0_ref, v1_ref, o_ref, vt):
    tokens = k0_ref.shape[0]
    @pl.when(pl.program_id(1) == 0)
    def _():
        vt[:, :tokens] = v0_ref[...].T
        vt[:, tokens:] = v1_ref[...].T
    q = q_ref[...] * jnp.bfloat16(0.125)
    lane = lax.broadcasted_iota(jnp.int32, q.shape, 1)
    outs = []
    for head in range(2):
        keep = (lane >= 64) if head else (lane < 64)
        qh = jnp.where(keep, q, jnp.zeros_like(q))
        s0 = lax.dot_general(k0_ref[...], qh, NT, preferred_element_type=jnp.float32)
        s1 = lax.dot_general(k1_ref[...], qh, NT, preferred_element_type=jnp.float32)
        peak = jnp.maximum(jnp.max(s0, axis=0, keepdims=True), jnp.max(s1, axis=0, keepdims=True))
        p0 = jnp.exp(s0 - peak)
        p1 = jnp.exp(s1 - peak)
        total = jnp.sum(p0, axis=0, keepdims=True) + jnp.sum(p1, axis=0, keepdims=True)
        vh = vt[64 * head:64 * head + 64, :]
        acc = jnp.dot(vh[:, :tokens], p0.astype(jnp.bfloat16), preferred_element_type=jnp.float32)
        acc = acc + jnp.dot(vh[:, tokens:], p1.astype(jnp.bfloat16), preferred_element_type=jnp.float32)
        outs.append(acc / total)
    o_ref[...] = jnp.concatenate(outs, axis=0).T.astype(o_ref.dtype)

def attend(query, keys, vals, other_keys, other_vals, block=512):
    tokens, width = query.shape
    kv = lambda p, b: (0, p)
    return pl.pallas_call(
        attend_kernel, grid=(width // 128, tokens // block),
        in_specs=[pl.BlockSpec((block, 128), lambda p, b: (b, p))] + [pl.BlockSpec((tokens, 128), kv)] * 4,
        out_specs=pl.BlockSpec((block, 128), lambda p, b: (b, p)),
        out_shape=jax.ShapeDtypeStruct((tokens, width), jnp.bfloat16),
        scratch_shapes=[pltpu.VMEM((128, 2 * tokens), jnp.bfloat16)],
        compiler_params=pltpu.CompilerParams(vmem_limit_bytes=60 * 1024 * 1024), name="attend",
    )(query, keys, other_keys, vals, other_vals)


def norm_rows(sums, scale, shift, count):
    channels = sums.shape[1]
    width = channels // GROUPS
    grouped = jnp.sum(sums.reshape(2, GROUPS, width), axis=-1)
    moments = (grouped + swap_cores(grouped)) / count
    mean = moments[0]
    inv_std = lax.rsqrt(moments[1] - mean * mean + NORM_EPS)
    return jnp.stack([jnp.repeat(mean, width), jnp.repeat(inv_std, width) * scale.astype(jnp.float32), shift.astype(jnp.float32)])


def channel_sums(half):
    wide = half.astype(jnp.float32)
    return jnp.stack([jnp.sum(wide, axis=(0, 1)), jnp.sum(wide * wide, axis=(0, 1))])


def edge_of(half, core):
    return swap_cores(jnp.where(core == 0, half[:, -1:], half[:, :1]))


def res_block(half, sums, time_vec, gn_scale, gn_shift, conv_w, norm_idx, conv_idx, core):
    count = 2 * half.shape[0] * half.shape[1] * (half.shape[2] // GROUPS)
    core_arg = core.reshape(1).astype(jnp.int32)
    norm = norm_rows(sums, gn_scale[norm_idx], gn_shift[norm_idx], count)
    hidden, sums = conv(core_arg, half, edge_of(half, core), norm, conv_w, conv_idx, time_vec[None])
    norm = norm_rows(sums, gn_scale[norm_idx + 1], gn_shift[norm_idx + 1], count)
    return conv(core_arg, hidden, edge_of(hidden, core), norm, conv_w, conv_idx + 1, half)


def attention_block(half, sums, scale, shift, w_qkv, w_out):
    rows, cols, channels = half.shape
    norm = norm_rows(sums, scale, shift, 2 * rows * cols * (channels // GROUPS))
    normed = ((half.astype(jnp.float32) - norm[0]) * norm[1] + norm[2]).astype(jnp.bfloat16).reshape(rows * cols, channels)
    flat = w_qkv.reshape(3, channels, channels)

    def project(weight):
        return jnp.dot(normed, weight, preferred_element_type=jnp.float32).astype(jnp.bfloat16)

    keys, vals = project(flat[1]), project(flat[2])
    other_keys, other_vals = swap_cores(keys), swap_cores(vals)
    query = project(flat[0])
    attended = attend(query, keys, vals, other_keys, other_vals)
    out = jnp.dot(attended, w_out.reshape(channels, channels), preferred_element_type=jnp.float32)
    return (half.astype(jnp.float32) + out.reshape(half.shape)).astype(jnp.bfloat16)


def solution(mesh):
    lat_spec = P("dp", "sp", "sp2", None)

    def local(x, time_emb, gn_scale, gn_shift, conv_w, time_w, w_qkv, w_out):
        y, core = place(lax.axis_index(SP))
        image = y * 4 + lax.axis_index(SP2)
        time_act = jax.nn.silu(time_emb.astype(jnp.float32)).astype(jnp.bfloat16)
        time_vecs = jnp.einsum("bt,stc->sbc", time_act, time_w, preferred_element_type=jnp.float32)
        time_vecs = lax.dynamic_index_in_dim(time_vecs, image, 1, keepdims=False)
        half = to_images(x)
        first, sums = res_block(half, channel_sums(half), time_vecs[0], gn_scale, gn_shift, conv_w, 0, 0, core)
        middle = attention_block(first, sums, gn_scale[2], gn_shift[2], w_qkv, w_out)
        last, _ = res_block(middle, channel_sums(middle), time_vecs[1], gn_scale, gn_shift, conv_w, 3, 2, core)
        return to_tiles(last)

    return jax.shard_map(local, mesh=mesh, in_specs=(lat_spec, P("dp", None), P(), P(), P(), P(), P(), P()), out_specs=lat_spec, check_vma=False)
```

```python
import functools

import jax
import jax.numpy as jnp
from jax import lax
from jax.experimental import pallas as pl
from jax.experimental.pallas import tpu as pltpu
from jax.sharding import PartitionSpec as P

GROUPS = 32
NORM_EPS = 1e-5
MESH = pl.DeviceIdType.MESH
SP, SP2 = "sp", "sp2"


def place(sp, cores=2):
    return sp // cores, lax.rem(sp, cores)


def to_images_kernel(x_ref, out_ref, stage, send_sem, recv_sem, self_sem):
    images, rows, cols, _ = x_ref.shape
    sp, z = lax.axis_index(SP), lax.axis_index(SP2)
    y, core = place(sp)
    mine = y * 4 + z
    to_core = z // 2
    own = to_core == core
    barrier = pltpu.get_barrier_semaphore()
    for s in range(8):
        src_sp, src_z = s // 2, 2 * core + s % 2

        @pl.when(jnp.logical_not((src_sp == sp) & (src_z == z)))
        def _():
            pl.semaphore_signal(barrier, inc=1, device_id={SP: src_sp, SP2: src_z}, device_id_type=MESH)

    pl.semaphore_wait(barrier, 8 - own.astype(jnp.int32))

    def piece(src_sp, src_z):
        return out_ref.at[pl.ds(src_sp * rows, rows), pl.ds(lax.rem(src_z, 2) * cols, cols), :]

    def send(i):
        return pltpu.make_async_remote_copy(
            src_ref=x_ref.at[i], dst_ref=piece(sp, z), send_sem=send_sem.at[i], recv_sem=recv_sem.at[sp * 2 + lax.rem(z, 2)],
            device_id={SP: (i // 4) * 2 + to_core, SP2: i % 4}, device_id_type=MESH)

    def is_self(i):
        return own & (mine == i)

    for i in range(images):
        @pl.when(jnp.logical_not(is_self(i)))
        def _():
            send(i).start()

    @pl.when(own)
    def _():
        load = pltpu.make_async_copy(x_ref.at[mine], stage, self_sem)
        load.start()
        load.wait()
        store = pltpu.make_async_copy(stage, piece(sp, z), self_sem)
        store.start()
        store.wait()

    for s in range(8):
        src_sp, src_z = s // 2, 2 * core + s % 2

        @pl.when(jnp.logical_not((src_sp == sp) & (src_z == z)))
        def _():
            pltpu.make_async_remote_copy(
                src_ref=x_ref.at[0], dst_ref=piece(src_sp, src_z), send_sem=send_sem.at[0], recv_sem=recv_sem.at[s],
                device_id={SP: src_sp, SP2: src_z}, device_id_type=MESH).wait_recv()

    for i in range(images):
        @pl.when(jnp.logical_not(is_self(i)))
        def _():
            send(i).wait_send()


def to_images(x):
    images, rows, cols, channels = x.shape
    return pl.pallas_call(
        to_images_kernel,
        out_shape=jax.ShapeDtypeStruct((4 * rows, 2 * cols, channels), x.dtype),
        in_specs=[pl.BlockSpec(memory_space=pl.ANY)],
        out_specs=pl.BlockSpec(memory_space=pl.ANY),
        scratch_shapes=[pltpu.VMEM((rows, cols, channels), x.dtype), pltpu.SemaphoreType.DMA((8,)), pltpu.SemaphoreType.DMA((8,)), pltpu.SemaphoreType.DMA],
        compiler_params=pltpu.CompilerParams(collective_id=0, has_side_effects=True),
        name="to_images",
    )(x)


def swap_cores(value):
    return lax.ppermute(value, SP, [(0, 1), (1, 0), (2, 3), (3, 2)])


def silu(v):
    return v / (1.0 + jnp.exp(-v))


def fill_act(core, h_ref, other_ref, norm_ref, act):
    rows, cols, channels = h_ref.shape
    mean, mult, shift = norm_ref[0:1, :], norm_ref[1:2, :], norm_ref[2:3, :]

    def activate(v):
        return silu((v.astype(jnp.float32) - mean) * mult + shift)

    zeros = jnp.zeros((cols, channels), jnp.bfloat16)
    for dx in range(3):
        act[dx, 0] = zeros
        act[dx, rows + 1] = zeros
    line = lax.broadcasted_iota(jnp.int32, (cols, channels), 0)

    def one_row(r, carry):
        u = activate(h_ref[r])
        edge = activate(other_ref[r])
        left = jnp.where(core == 1, edge, 0.0)
        right = jnp.where(core == 0, edge, 0.0)
        act[1, r + 1] = u.astype(jnp.bfloat16)
        act[0, r + 1] = jnp.where(line == 0, left, pltpu.roll(u, 1, 0)).astype(jnp.bfloat16)
        act[2, r + 1] = jnp.where(line == cols - 1, right, pltpu.roll(u, cols - 1, 0)).astype(jnp.bfloat16)
        return carry

    lax.fori_loop(0, rows, one_row, 0)


def taps(act, w_ref, rows, cols, channels):
    total = None
    for k in range(9):
        lhs = act[k % 3, pl.ds(k // 3, rows)].reshape(rows * cols, channels)
        part = jnp.dot(lhs, w_ref[k // 3, k % 3], preferred_element_type=jnp.float32)
        total = part if total is None else total + part
    return total


def conv_kernel(residual, h_ref, other_ref, norm_ref, w_ref, add_ref, out_ref, sums_ref, edge_ref, act):
    rows, cols, channels = h_ref.shape
    width = w_ref.shape[-1]
    _, core = place(lax.axis_index(SP))

    @pl.when(pl.program_id(0) == 0)
    def _():
        fill_act(core, h_ref, other_ref, norm_ref, act)

    full = taps(act, w_ref, rows, cols, channels)
    full = full + (add_ref[...].reshape(rows * cols, width).astype(jnp.float32) if residual else add_ref[...])
    half = full.astype(jnp.bfloat16)
    out_ref[...] = half.reshape(rows, cols, width)
    kept = half.astype(jnp.float32)
    sums_ref[...] = jnp.concatenate([jnp.sum(kept, axis=0, keepdims=True), jnp.sum(kept * kept, axis=0, keepdims=True)], axis=0)

    @pl.when(core == 0)
    def _():
        edge_ref[...] = out_ref[:, cols - 1:, :]

    @pl.when(core == 1)
    def _():
        edge_ref[...] = out_ref[:, :1, :]


def conv_specs(rows, cols, channels, j, nb, residual):
    whole = lambda *s: pl.BlockSpec(s, lambda n: (0,) * len(s))
    add = pl.BlockSpec((rows, cols, nb), lambda n: (0, 0, n)) if residual else pl.BlockSpec((1, nb), lambda n: (0, n))
    return [whole(rows, cols, channels), whole(rows, 1, channels), whole(3, channels), pl.BlockSpec((None, 3, 3, channels, nb), lambda n: (j, 0, 0, 0, n)), add]


def conv_cost(rows, cols, channels):
    return pl.CostEstimate(flops=18 * rows * cols * channels * channels, bytes_accessed=18 * channels * channels, transcendentals=rows * cols * channels)


def conv(h, other, norm, w, j, add, nb=256):
    rows, cols, channels = h.shape
    return pl.pallas_call(
        functools.partial(conv_kernel, add.ndim == 3),
        grid=(channels // nb,),
        in_specs=conv_specs(rows, cols, channels, j, nb, add.ndim == 3),
        out_specs=[pl.BlockSpec((rows, cols, nb), lambda n: (0, 0, n)), pl.BlockSpec((2, nb), lambda n: (0, n)), pl.BlockSpec((rows, 1, nb), lambda n: (0, 0, n))],
        out_shape=[jax.ShapeDtypeStruct((rows, cols, channels), jnp.bfloat16), jax.ShapeDtypeStruct((2, channels), jnp.float32), jax.ShapeDtypeStruct((rows, 1, channels), jnp.bfloat16)],
        scratch_shapes=[pltpu.VMEM((3, rows + 2, cols, channels), jnp.bfloat16)],
        compiler_params=pltpu.CompilerParams(vmem_limit_bytes=62 * 1024 * 1024),
        cost_estimate=conv_cost(rows, cols, channels),
        name="conv",
    )(h, other, norm, w, add)


def conv_out_kernel(h_ref, other_ref, norm_ref, w_ref, add_ref, out_ref, act, done, send_sem, recv_sem, self_sem):
    rows, cols, channels = h_ref.shape
    images, trows, tcols, _ = out_ref.shape
    width = w_ref.shape[-1]
    n, chunks = pl.program_id(0), pl.num_programs(0)
    sp, z = lax.axis_index(SP), lax.axis_index(SP2)
    y, core = place(sp)
    mine = y * 4 + z
    from_core = z // 2
    own = from_core == core

    @pl.when(n == 0)
    def _():
        barrier = pltpu.get_barrier_semaphore()
        for i in range(images):
            @pl.when(jnp.logical_not(own & (mine == i)))
            def _():
                pl.semaphore_signal(barrier, inc=1, device_id={SP: (i // 4) * 2 + from_core, SP2: i % 4}, device_id_type=MESH)

        fill_act(core, h_ref, other_ref, norm_ref, act)
        pl.semaphore_wait(barrier, 8 - own.astype(jnp.int32))

    full = taps(act, w_ref, rows, cols, channels) + add_ref[...].reshape(rows * cols, width).astype(jnp.float32)
    done[n] = full.astype(jnp.bfloat16).reshape(rows, cols, width)

    def lanes(c):
        return pl.ds(pl.multiple_of(c * width, width), width)

    def piece(c, dst_sp, dst_z):
        return done.at[c, pl.ds(dst_sp * trows, trows), pl.ds(pl.multiple_of(lax.rem(dst_z, 2) * tcols, tcols), tcols), :]

    def send(c, s):
        dst_sp, dst_z = s // 2, 2 * core + s % 2
        return pltpu.make_async_remote_copy(
            src_ref=piece(c, dst_sp, dst_z), dst_ref=out_ref.at[mine, :, :, lanes(c)], send_sem=send_sem.at[c, s], recv_sem=recv_sem.at[c, mine],
            device_id={SP: dst_sp, SP2: dst_z}, device_id_type=MESH)

    def keep(c):
        return pltpu.make_async_copy(piece(c, sp, z), out_ref.at[mine, :, :, lanes(c)], self_sem.at[c])

    def is_self(s):
        return (s // 2 == sp) & (2 * core + s % 2 == z)

    for s in range(8):
        @pl.when(jnp.logical_not(is_self(s)))
        def _():
            send(n, s).start()

    @pl.when(own)
    def _():
        keep(n).start()

    @pl.when(n == chunks - 1)
    def _():
        def drain(c, carry):
            for i in range(images):
                @pl.when(jnp.logical_not(own & (mine == i)))
                def _():
                    pltpu.make_async_remote_copy(
                        src_ref=piece(c, 0, 0), dst_ref=out_ref.at[i, :, :, lanes(c)], send_sem=send_sem.at[c, 0], recv_sem=recv_sem.at[c, i],
                        device_id={SP: (i // 4) * 2 + from_core, SP2: i % 4}, device_id_type=MESH).wait_recv()

            for s in range(8):
                @pl.when(jnp.logical_not(is_self(s)))
                def _():
                    send(c, s).wait_send()

            @pl.when(own)
            def _():
                keep(c).wait()
            return carry

        lax.fori_loop(0, channels // width, drain, 0)


def conv_out(h, other, norm, w, j, add, nb=256):
    rows, cols, channels = h.shape
    chunks = channels // nb
    return pl.pallas_call(
        conv_out_kernel,
        grid=(chunks,),
        in_specs=conv_specs(rows, cols, channels, j, nb, True),
        out_specs=pl.BlockSpec(memory_space=pl.ANY),
        out_shape=jax.ShapeDtypeStruct((8, rows // 4, cols // 2, channels), jnp.bfloat16),
        scratch_shapes=[pltpu.VMEM((3, rows + 2, cols, channels), jnp.bfloat16), pltpu.VMEM((chunks, rows, cols, nb), jnp.bfloat16),
                        pltpu.SemaphoreType.DMA((chunks, 8)), pltpu.SemaphoreType.DMA((chunks, 8)), pltpu.SemaphoreType.DMA((chunks,))],
        compiler_params=pltpu.CompilerParams(collective_id=1, has_side_effects=True, vmem_limit_bytes=62 * 1024 * 1024),
        cost_estimate=conv_cost(rows, cols, channels),
        name="conv_out",
    )(h, other, norm, w, add)


NT = (((1,), (1,)), ((), ()))

def attend_kernel(q_ref, k0_ref, k1_ref, v0_ref, v1_ref, o_ref, vt):
    tokens = k0_ref.shape[0]
    @pl.when(pl.program_id(1) == 0)
    def _():
        vt[:, :tokens] = v0_ref[...].T
        vt[:, tokens:] = v1_ref[...].T
    q = q_ref[...] * jnp.bfloat16(0.125)
    lane = lax.broadcasted_iota(jnp.int32, q.shape, 1)
    outs = []
    for head in range(2):
        keep = (lane >= 64) if head else (lane < 64)
        qh = jnp.where(keep, q, jnp.zeros_like(q))
        s0 = lax.dot_general(k0_ref[...], qh, NT, preferred_element_type=jnp.float32)
        s1 = lax.dot_general(k1_ref[...], qh, NT, preferred_element_type=jnp.float32)
        peak = jnp.maximum(jnp.max(s0, axis=0, keepdims=True), jnp.max(s1, axis=0, keepdims=True))
        p0 = jnp.exp(s0 - peak)
        p1 = jnp.exp(s1 - peak)
        total = jnp.sum(p0, axis=0, keepdims=True) + jnp.sum(p1, axis=0, keepdims=True)
        vh = vt[64 * head:64 * head + 64, :]
        acc = jnp.dot(vh[:, :tokens], p0.astype(jnp.bfloat16), preferred_element_type=jnp.float32)
        acc = acc + jnp.dot(vh[:, tokens:], p1.astype(jnp.bfloat16), preferred_element_type=jnp.float32)
        outs.append(acc / total)
    o_ref[...] = jnp.concatenate(outs, axis=0).T.astype(o_ref.dtype)

def attend(query, keys, vals, other_keys, other_vals, block=512):
    tokens, width = query.shape
    kv = lambda p, b: (0, p)
    return pl.pallas_call(
        attend_kernel, grid=(width // 128, tokens // block),
        in_specs=[pl.BlockSpec((block, 128), lambda p, b: (b, p))] + [pl.BlockSpec((tokens, 128), kv)] * 4,
        out_specs=pl.BlockSpec((block, 128), lambda p, b: (b, p)),
        out_shape=jax.ShapeDtypeStruct((tokens, width), jnp.bfloat16),
        scratch_shapes=[pltpu.VMEM((128, 2 * tokens), jnp.bfloat16)],
        compiler_params=pltpu.CompilerParams(vmem_limit_bytes=60 * 1024 * 1024), name="attend",
    )(query, keys, other_keys, vals, other_vals)


def norm_rows(sums, scale, shift, count):
    channels = sums.shape[1]
    width = channels // GROUPS
    grouped = jnp.sum(sums.reshape(2, GROUPS, width), axis=-1)
    moments = (grouped + swap_cores(grouped)) / count
    mean = moments[0]
    inv_std = lax.rsqrt(moments[1] - mean * mean + NORM_EPS)
    return jnp.stack([jnp.repeat(mean, width), jnp.repeat(inv_std, width) * scale.astype(jnp.float32), shift.astype(jnp.float32)])


def channel_sums(half):
    wide = half.astype(jnp.float32)
    return jnp.stack([jnp.sum(wide, axis=(0, 1)), jnp.sum(wide * wide, axis=(0, 1))])


def edge_of(half, core):
    return swap_cores(jnp.where(core == 0, half[:, -1:], half[:, :1]))


def res_block(half, sums, time_vec, gn_scale, gn_shift, conv_w, norm_idx, conv_idx, core, last):
    count = 2 * half.shape[0] * half.shape[1] * (half.shape[2] // GROUPS)
    norm = norm_rows(sums, gn_scale[norm_idx], gn_shift[norm_idx], count)
    hidden, sums, edge = conv(half, edge_of(half, core), norm, conv_w, conv_idx, time_vec[None])
    norm = norm_rows(sums, gn_scale[norm_idx + 1], gn_shift[norm_idx + 1], count)
    return last(hidden, swap_cores(edge), norm, conv_w, conv_idx + 1, half)


def attention_block(half, sums, scale, shift, w_qkv, w_out):
    rows, cols, channels = half.shape
    norm = norm_rows(sums, scale, shift, 2 * rows * cols * (channels // GROUPS))
    normed = ((half.astype(jnp.float32) - norm[0]) * norm[1] + norm[2]).astype(jnp.bfloat16).reshape(rows * cols, channels)
    flat = w_qkv.reshape(3, channels, channels)

    def project(weight):
        return jnp.dot(normed, weight, preferred_element_type=jnp.float32).astype(jnp.bfloat16)

    keys, vals = project(flat[1]), project(flat[2])
    other_keys, other_vals = swap_cores(keys), swap_cores(vals)
    query = project(flat[0])
    attended = attend(query, keys, vals, other_keys, other_vals)
    out = jnp.dot(attended, w_out.reshape(channels, channels), preferred_element_type=jnp.float32)
    return (half.astype(jnp.float32) + out.reshape(half.shape)).astype(jnp.bfloat16)


def solution(mesh):
    lat_spec = P("dp", "sp", "sp2", None)

    def local(x, time_emb, gn_scale, gn_shift, conv_w, time_w, w_qkv, w_out):
        y, core = place(lax.axis_index(SP))
        image = y * 4 + lax.axis_index(SP2)
        time_act = jax.nn.silu(time_emb.astype(jnp.float32)).astype(jnp.bfloat16)
        time_vecs = jnp.einsum("bt,stc->sbc", time_act, time_w, preferred_element_type=jnp.float32)
        time_vecs = lax.dynamic_index_in_dim(time_vecs, image, 1, keepdims=False)
        half = to_images(x)
        first, sums, _ = res_block(half, channel_sums(half), time_vecs[0], gn_scale, gn_shift, conv_w, 0, 0, core, conv)
        middle = attention_block(first, sums, gn_scale[2], gn_shift[2], w_qkv, w_out)
        return res_block(middle, channel_sums(middle), time_vecs[1], gn_scale, gn_shift, conv_w, 3, 2, core, conv_out)

    return jax.shard_map(local, mesh=mesh, in_specs=(lat_spec, P("dp", None), P(), P(), P(), P(), P(), P()), out_specs=lat_spec, check_vma=False)
```

```python
import functools

import jax
import jax.numpy as jnp
from jax import lax
from jax.experimental import pallas as pl
from jax.experimental.pallas import tpu as pltpu
from jax.sharding import PartitionSpec as P

GROUPS = 32
NORM_EPS = 1e-5
MESH = pl.DeviceIdType.MESH
SP, SP2 = "sp", "sp2"


def place(sp, cores=2):
    return sp // cores, lax.rem(sp, cores)


def swap_cores(value):
    return lax.ppermute(value, SP, [(0, 1), (1, 0), (2, 3), (3, 2)])


def group_rows(sums, scale, shift, count):
    channels = sums.shape[1]
    width = channels // GROUPS

    def member(shape, channel_dim):
        channel = lax.broadcasted_iota(jnp.int32, shape, channel_dim).astype(jnp.float32)
        group = lax.broadcasted_iota(jnp.int32, shape, 1 - channel_dim).astype(jnp.float32)
        return (jnp.floor((channel + 0.5) / width) == group).astype(jnp.float32)

    exact = lax.Precision.HIGHEST
    moments = jnp.dot(sums, member((channels, 128), 0), precision=exact, preferred_element_type=jnp.float32) / count
    mean = moments[0:1]
    inv_std = lax.rsqrt(moments[1:2] - mean * mean + NORM_EPS)
    spread = jnp.dot(jnp.concatenate([mean, inv_std], axis=0), member((128, channels), 1), precision=exact, preferred_element_type=jnp.float32)
    return jnp.concatenate([spread[0:1], spread[1:2] * scale.astype(jnp.float32), shift.astype(jnp.float32)], axis=0)


def silu(v):
    return v / (1.0 + jnp.exp(-v))


def fill_act(core, h_ref, other_ref, norm_ref, act):
    rows, cols, channels = h_ref.shape
    mean, mult, shift = norm_ref[0:1, :], norm_ref[1:2, :], norm_ref[2:3, :]

    def activate(v):
        return silu((v.astype(jnp.float32) - mean) * mult + shift)

    zeros = jnp.zeros((cols, channels), jnp.bfloat16)
    for dx in range(3):
        act[dx, 0] = zeros
        act[dx, rows + 1] = zeros
    line = lax.broadcasted_iota(jnp.int32, (cols, channels), 0)

    def one_row(r, carry):
        u = activate(h_ref[r])
        edge = activate(other_ref[r])
        left = jnp.where(core == 1, edge, 0.0)
        right = jnp.where(core == 0, edge, 0.0)
        act[1, r + 1] = u.astype(jnp.bfloat16)
        act[0, r + 1] = jnp.where(line == 0, left, pltpu.roll(u, 1, 0)).astype(jnp.bfloat16)
        act[2, r + 1] = jnp.where(line == cols - 1, right, pltpu.roll(u, cols - 1, 0)).astype(jnp.bfloat16)
        return carry

    lax.fori_loop(0, rows, one_row, 0)


def taps(act, w_ref, rows, cols, channels):
    total = None
    for k in range(9):
        lhs = act[k % 3, pl.ds(k // 3, rows)].reshape(rows * cols, channels)
        part = jnp.dot(lhs, w_ref[k // 3, k % 3], preferred_element_type=jnp.float32)
        total = part if total is None else total + part
    return total


def conv_kernel(residual, norm_idx, h_ref, other_ref, own_ref, theirs_ref, scale_ref, shift_ref, w_ref, add_ref, out_ref, sums_ref, edge_ref, act, norm_ref):
    rows, cols, channels = h_ref.shape
    width = w_ref.shape[-1]
    _, core = place(lax.axis_index(SP))

    @pl.when(pl.program_id(0) == 0)
    def _():
        count = 2 * rows * cols * (channels // GROUPS)
        norm_ref[...] = group_rows(own_ref[...] + theirs_ref[...], scale_ref[norm_idx:norm_idx + 1, :], shift_ref[norm_idx:norm_idx + 1, :], count)
        fill_act(core, h_ref, other_ref, norm_ref, act)

    full = taps(act, w_ref, rows, cols, channels)
    full = full + (add_ref[...].reshape(rows * cols, width).astype(jnp.float32) if residual else add_ref[...])
    half = full.astype(jnp.bfloat16)
    out_ref[...] = half.reshape(rows, cols, width)
    kept = half.astype(jnp.float32)
    sums_ref[...] = jnp.concatenate([jnp.sum(kept, axis=0, keepdims=True), jnp.sum(kept * kept, axis=0, keepdims=True)], axis=0)

    @pl.when(core == 0)
    def _():
        edge_ref[...] = out_ref[:, cols - 1:, :]

    @pl.when(core == 1)
    def _():
        edge_ref[...] = out_ref[:, :1, :]


def conv_specs(rows, cols, channels, j, nb, residual):
    whole = lambda *s: pl.BlockSpec(s, lambda n: (0,) * len(s))
    add = pl.BlockSpec((rows, cols, nb), lambda n: (0, 0, n)) if residual else pl.BlockSpec((1, nb), lambda n: (0, n))
    return [whole(rows, cols, channels), whole(rows, 1, channels), whole(2, channels), whole(2, channels), whole(5, channels), whole(5, channels), pl.BlockSpec((None, 3, 3, channels, nb), lambda n: (j, 0, 0, 0, n)), add]


def conv_cost(rows, cols, channels):
    return pl.CostEstimate(flops=18 * rows * cols * channels * channels, bytes_accessed=18 * channels * channels, transcendentals=rows * cols * channels)


def conv(h, other, own, theirs, scale, shift, norm_idx, w, j, add, nb=256):
    rows, cols, channels = h.shape
    return pl.pallas_call(
        functools.partial(conv_kernel, add.ndim == 3, norm_idx),
        grid=(channels // nb,),
        in_specs=conv_specs(rows, cols, channels, j, nb, add.ndim == 3),
        out_specs=[pl.BlockSpec((rows, cols, nb), lambda n: (0, 0, n)), pl.BlockSpec((2, nb), lambda n: (0, n)), pl.BlockSpec((rows, 1, nb), lambda n: (0, 0, n))],
        out_shape=[jax.ShapeDtypeStruct((rows, cols, channels), jnp.bfloat16), jax.ShapeDtypeStruct((2, channels), jnp.float32), jax.ShapeDtypeStruct((rows, 1, channels), jnp.bfloat16)],
        scratch_shapes=[pltpu.VMEM((3, rows + 2, cols, channels), jnp.bfloat16), pltpu.VMEM((3, channels), jnp.float32)],
        compiler_params=pltpu.CompilerParams(vmem_limit_bytes=62 * 1024 * 1024),
        cost_estimate=conv_cost(rows, cols, channels),
        name="conv",
    )(h, other, own, theirs, scale, shift, w, add)


def conv_in_kernel(x_ref, scale_ref, shift_ref, add_ref, w_ref, out_ref, half_ref, sums_ref, edge_ref,
                   tile, raw, beside, weights, act, acc, stats, heard, norm_ref,
                   tile_sem, w_sem, send_sem, recv_sem, self_sem, tell_sem, hear_sem, lend_sem, borrow_sem, keep_sem):
    images, trows, tcols, channels = x_ref.shape
    chunks, rows, cols, width = raw.shape
    sp, z = lax.axis_index(SP), lax.axis_index(SP2)
    y, core = place(sp)
    mine = y * 4 + z
    to_core = z // 2
    own = to_core == core
    me = sp * 4 + z
    load = pltpu.make_async_copy(x_ref, tile, tile_sem)
    load.start()
    barrier = pltpu.get_barrier_semaphore()
    for d in range(16):
        @pl.when(me != d)
        def _():
            pl.semaphore_signal(barrier, inc=1, device_id={SP: d // 4, SP2: d % 4}, device_id_type=MESH)

    def weight(c):
        return pltpu.make_async_copy(w_ref.at[0, :, :, pl.ds(pl.multiple_of(c * width, width), width), :], weights.at[c], w_sem.at[c])

    def lanes(c):
        return pl.ds(pl.multiple_of(c * width, width), width)

    def piece(c, src_sp, src_z):
        return raw.at[c, pl.ds(src_sp * trows, trows), pl.ds(pl.multiple_of(lax.rem(src_z, 2) * tcols, tcols), tcols), :]

    def send(c, i):
        return pltpu.make_async_remote_copy(
            src_ref=x_ref.at[i, :, :, lanes(c)], dst_ref=piece(c, sp, z), send_sem=send_sem.at[c, i], recv_sem=recv_sem.at[c, sp * 2 + lax.rem(z, 2)],
            device_id={SP: (i // 4) * 2 + to_core, SP2: i % 4}, device_id_type=MESH)

    def place_own(c):
        return pltpu.make_async_copy(x_ref.at[mine, :, :, lanes(c)], piece(c, sp, z), self_sem.at[c])

    def is_self(i):
        return own & (mine == i)

    def start_chunk(c):
        for i in range(images):
            @pl.when(jnp.logical_not(is_self(i)))
            def _():
                send(c, i).start()

        @pl.when(own)
        def _():
            place_own(c).start()

    def tell(i, k):
        return pltpu.make_async_remote_copy(
            src_ref=stats.at[i], dst_ref=heard.at[me], send_sem=tell_sem.at[i, k], recv_sem=hear_sem.at[me],
            device_id={SP: (i // 4) * 2 + k, SP2: i % 4}, device_id_type=MESH)

    pl.semaphore_wait(barrier, 15)
    start_chunk(0)
    for c in range(chunks):
        weight(c).start()
    load.wait()

    def sum_image(i, carry):
        wide = tile[i].reshape(trows * tcols, channels).astype(jnp.float32)
        stats[i] = jnp.concatenate([jnp.sum(wide, axis=0, keepdims=True), jnp.sum(wide * wide, axis=0, keepdims=True)], axis=0)
        return carry

    lax.fori_loop(0, images, sum_image, 0)
    for i in range(images):
        for k in range(2):
            @pl.when(jnp.logical_not((mine == i) & (core == k)))
            def _():
                tell(i, k).start()

    def start_rest(c, carry):
        start_chunk(c)
        return carry

    lax.fori_loop(1, chunks, start_rest, 0)
    total = stats[mine]
    for d in range(16):
        @pl.when(me != d)
        def _():
            pltpu.make_async_remote_copy(
                src_ref=stats.at[0], dst_ref=heard.at[d], send_sem=tell_sem.at[0, 0], recv_sem=hear_sem.at[d],
                device_id={SP: d // 4, SP2: d % 4}, device_id_type=MESH).wait_recv()

        total = total + jnp.where(me != d, heard[d], 0.0)
    count = 2 * rows * cols * (channels // GROUPS)
    norm_ref[...] = group_rows(total, scale_ref[0:1, :], shift_ref[0:1, :], count)
    zeros = jnp.zeros((cols, width), jnp.bfloat16)
    for dx in range(3):
        act[dx, 0] = zeros
        act[dx, rows + 1] = zeros
    line = lax.broadcasted_iota(jnp.int32, (cols, width), 0)
    band = beside.shape[2]

    def lend(c):
        first = pl.multiple_of((1 - core) * (cols - band), band)
        return pltpu.make_async_remote_copy(
            src_ref=raw.at[c, :, pl.ds(first, band), :], dst_ref=beside.at[c], send_sem=lend_sem.at[c], recv_sem=borrow_sem.at[c],
            device_id={SP: y * 2 + 1 - core}, device_id_type=MESH)

    def keep_raw(c):
        return pltpu.make_async_copy(raw.at[c], half_ref.at[:, :, lanes(c)], keep_sem.at[c])

    def one_chunk(c, carry):
        for s in range(8):
            src_sp, src_z = s // 2, 2 * core + s % 2

            @pl.when(jnp.logical_not((src_sp == sp) & (src_z == z)))
            def _():
                pltpu.make_async_remote_copy(
                    src_ref=x_ref.at[0, :, :, lanes(c)], dst_ref=piece(c, src_sp, src_z), send_sem=send_sem.at[c, 0], recv_sem=recv_sem.at[c, s],
                    device_id={SP: src_sp, SP2: src_z}, device_id_type=MESH).wait_recv()

        @pl.when(own)
        def _():
            place_own(c).wait()

        lend(c).start()
        keep_raw(c).start()
        mean, mult, shift = norm_ref[0:1, lanes(c)], norm_ref[1:2, lanes(c)], norm_ref[2:3, lanes(c)]

        def activate(v):
            return silu((v.astype(jnp.float32) - mean) * mult + shift)

        lend(c).wait_recv()

        def one_row(r, carry2):
            u = activate(raw[c, r])
            left = jnp.where(core == 1, activate(beside[c, r, band - 1:band, :]), 0.0)
            right = jnp.where(core == 0, activate(beside[c, r, 0:1, :]), 0.0)
            act[1, r + 1] = u.astype(jnp.bfloat16)
            act[0, r + 1] = jnp.where(line == 0, left, pltpu.roll(u, 1, 0)).astype(jnp.bfloat16)
            act[2, r + 1] = jnp.where(line == cols - 1, right, pltpu.roll(u, cols - 1, 0)).astype(jnp.bfloat16)
            return carry2

        lax.fori_loop(0, rows, one_row, 0)
        weight(c).wait()

        def one_block(n, carry2):
            part = None
            for k in range(9):
                lhs = act[k % 3, pl.ds(k // 3, rows)].reshape(rows * cols, width)
                dot = jnp.dot(lhs, weights[c, k // 3, k % 3, :, lanes(n)], preferred_element_type=jnp.float32)
                part = dot if part is None else part + dot

            @pl.when(c == 0)
            def _():
                acc[n] = part

            @pl.when(c > 0)
            def _():
                acc[n] += part
            return carry2

        lax.fori_loop(0, chunks, one_block, 0)
        return carry

    lax.fori_loop(0, chunks, one_chunk, 0)
    for n in range(chunks):
        cut = slice(n * width, (n + 1) * width)
        half = (acc[n] + add_ref[:, cut]).astype(jnp.bfloat16)
        out_ref[:, :, cut] = half.reshape(rows, cols, width)
        kept = half.astype(jnp.float32)
        sums_ref[:, cut] = jnp.concatenate([jnp.sum(kept, axis=0, keepdims=True), jnp.sum(kept * kept, axis=0, keepdims=True)], axis=0)

    @pl.when(core == 0)
    def _():
        edge_ref[...] = out_ref[:, cols - 1:, :]

    @pl.when(core == 1)
    def _():
        edge_ref[...] = out_ref[:, :1, :]

    def drain(c, carry):
        for i in range(images):
            @pl.when(jnp.logical_not(is_self(i)))
            def _():
                send(c, i).wait_send()

        lend(c).wait_send()
        keep_raw(c).wait()
        return carry

    lax.fori_loop(0, chunks, drain, 0)
    for i in range(images):
        for k in range(2):
            @pl.when(jnp.logical_not((mine == i) & (core == k)))
            def _():
                tell(i, k).wait_send()


def conv_in(x, scale, shift, add, w, width=256, band=16):
    images, trows, tcols, channels = x.shape
    rows, cols, chunks = 4 * trows, 2 * tcols, channels // width
    vmem, hbm = pl.BlockSpec(memory_space=pltpu.VMEM), pl.BlockSpec(memory_space=pl.ANY)
    dma = pltpu.SemaphoreType.DMA
    shape = jax.ShapeDtypeStruct
    return pl.pallas_call(
        conv_in_kernel,
        in_specs=[hbm, vmem, vmem, vmem, hbm],
        out_specs=[vmem, hbm, vmem, vmem],
        out_shape=[shape((rows, cols, channels), jnp.bfloat16), shape((rows, cols, channels), jnp.bfloat16), shape((2, channels), jnp.float32), shape((rows, 1, channels), jnp.bfloat16)],
        scratch_shapes=[
            pltpu.VMEM(x.shape, jnp.bfloat16), pltpu.VMEM((chunks, rows, cols, width), jnp.bfloat16), pltpu.VMEM((chunks, rows, band, width), jnp.bfloat16),
            pltpu.VMEM((chunks, 3, 3, width, channels), jnp.bfloat16), pltpu.VMEM((3, rows + 2, cols, width), jnp.bfloat16), pltpu.VMEM((chunks, rows * cols, width), jnp.float32),
            pltpu.VMEM((images, 2, channels), jnp.float32), pltpu.VMEM((16, 2, channels), jnp.float32), pltpu.VMEM((3, channels), jnp.float32),
            dma, dma((chunks,)), dma((chunks, 8)), dma((chunks, 8)), dma((chunks,)), dma((8, 2)), dma((16,)), dma((chunks,)), dma((chunks,)), dma((chunks,))],
        compiler_params=pltpu.CompilerParams(collective_id=0, has_side_effects=True, vmem_limit_bytes=63 * 1024 * 1024),
        cost_estimate=conv_cost(rows, cols, channels),
        name="conv_in",
    )(x, scale, shift, add, w)


def conv_out_kernel(norm_idx, h_ref, other_ref, own_ref, theirs_ref, scale_ref, shift_ref, w_ref, add_ref, out_ref, act, norm_ref, done, send_sem, recv_sem, self_sem):
    rows, cols, channels = h_ref.shape
    images, trows, tcols, _ = out_ref.shape
    width = w_ref.shape[-1]
    n, chunks = pl.program_id(0), pl.num_programs(0)
    sp, z = lax.axis_index(SP), lax.axis_index(SP2)
    y, core = place(sp)
    mine = y * 4 + z
    from_core = z // 2
    own = from_core == core

    @pl.when(n == 0)
    def _():
        barrier = pltpu.get_barrier_semaphore()
        for i in range(images):
            @pl.when(jnp.logical_not(own & (mine == i)))
            def _():
                pl.semaphore_signal(barrier, inc=1, device_id={SP: (i // 4) * 2 + from_core, SP2: i % 4}, device_id_type=MESH)

        count = 2 * rows * cols * (channels // GROUPS)
        norm_ref[...] = group_rows(own_ref[...] + theirs_ref[...], scale_ref[norm_idx:norm_idx + 1, :], shift_ref[norm_idx:norm_idx + 1, :], count)
        fill_act(core, h_ref, other_ref, norm_ref, act)
        pl.semaphore_wait(barrier, 8 - own.astype(jnp.int32))

    full = taps(act, w_ref, rows, cols, channels) + add_ref[...].reshape(rows * cols, width).astype(jnp.float32)
    done[n] = full.astype(jnp.bfloat16).reshape(rows, cols, width)

    def lanes(c):
        return pl.ds(pl.multiple_of(c * width, width), width)

    def piece(c, dst_sp, dst_z):
        return done.at[c, pl.ds(dst_sp * trows, trows), pl.ds(pl.multiple_of(lax.rem(dst_z, 2) * tcols, tcols), tcols), :]

    def send(c, s):
        dst_sp, dst_z = s // 2, 2 * core + s % 2
        return pltpu.make_async_remote_copy(
            src_ref=piece(c, dst_sp, dst_z), dst_ref=out_ref.at[mine, :, :, lanes(c)], send_sem=send_sem.at[c, s], recv_sem=recv_sem.at[c, mine],
            device_id={SP: dst_sp, SP2: dst_z}, device_id_type=MESH)

    def keep(c):
        return pltpu.make_async_copy(piece(c, sp, z), out_ref.at[mine, :, :, lanes(c)], self_sem.at[c])

    def is_self(s):
        return (s // 2 == sp) & (2 * core + s % 2 == z)

    for s in range(8):
        @pl.when(jnp.logical_not(is_self(s)))
        def _():
            send(n, s).start()

    @pl.when(own)
    def _():
        keep(n).start()

    @pl.when(n == chunks - 1)
    def _():
        def drain(c, carry):
            for i in range(images):
                @pl.when(jnp.logical_not(own & (mine == i)))
                def _():
                    pltpu.make_async_remote_copy(
                        src_ref=piece(c, 0, 0), dst_ref=out_ref.at[i, :, :, lanes(c)], send_sem=send_sem.at[c, 0], recv_sem=recv_sem.at[c, i],
                        device_id={SP: (i // 4) * 2 + from_core, SP2: i % 4}, device_id_type=MESH).wait_recv()

            for s in range(8):
                @pl.when(jnp.logical_not(is_self(s)))
                def _():
                    send(c, s).wait_send()

            @pl.when(own)
            def _():
                keep(c).wait()
            return carry

        lax.fori_loop(0, channels // width, drain, 0)


def conv_out(h, other, own, theirs, scale, shift, norm_idx, w, j, add, nb=256):
    rows, cols, channels = h.shape
    chunks = channels // nb
    return pl.pallas_call(
        functools.partial(conv_out_kernel, norm_idx),
        grid=(chunks,),
        in_specs=conv_specs(rows, cols, channels, j, nb, True),
        out_specs=pl.BlockSpec(memory_space=pl.ANY),
        out_shape=jax.ShapeDtypeStruct((8, rows // 4, cols // 2, channels), jnp.bfloat16),
        scratch_shapes=[pltpu.VMEM((3, rows + 2, cols, channels), jnp.bfloat16), pltpu.VMEM((3, channels), jnp.float32), pltpu.VMEM((chunks, rows, cols, nb), jnp.bfloat16),
                        pltpu.SemaphoreType.DMA((chunks, 8)), pltpu.SemaphoreType.DMA((chunks, 8)), pltpu.SemaphoreType.DMA((chunks,))],
        compiler_params=pltpu.CompilerParams(collective_id=1, has_side_effects=True, vmem_limit_bytes=62 * 1024 * 1024),
        cost_estimate=conv_cost(rows, cols, channels),
        name="conv_out",
    )(h, other, own, theirs, scale, shift, w, add)


NT = (((1,), (1,)), ((), ()))

def attend_kernel(q_ref, k0_ref, k1_ref, v0_ref, v1_ref, o_ref, vt):
    tokens = k0_ref.shape[0]
    @pl.when(pl.program_id(1) == 0)
    def _():
        vt[:, :tokens] = v0_ref[...].T
        vt[:, tokens:] = v1_ref[...].T
    q = q_ref[...] * jnp.bfloat16(0.125)
    lane = lax.broadcasted_iota(jnp.int32, q.shape, 1)
    outs = []
    for head in range(2):
        keep = (lane >= 64) if head else (lane < 64)
        qh = jnp.where(keep, q, jnp.zeros_like(q))
        s0 = lax.dot_general(k0_ref[...], qh, NT, preferred_element_type=jnp.float32)
        s1 = lax.dot_general(k1_ref[...], qh, NT, preferred_element_type=jnp.float32)
        peak = jnp.maximum(jnp.max(s0, axis=0, keepdims=True), jnp.max(s1, axis=0, keepdims=True))
        p0 = jnp.exp(s0 - peak)
        p1 = jnp.exp(s1 - peak)
        total = jnp.sum(p0, axis=0, keepdims=True) + jnp.sum(p1, axis=0, keepdims=True)
        vh = vt[64 * head:64 * head + 64, :]
        acc = jnp.dot(vh[:, :tokens], p0.astype(jnp.bfloat16), preferred_element_type=jnp.float32)
        acc = acc + jnp.dot(vh[:, tokens:], p1.astype(jnp.bfloat16), preferred_element_type=jnp.float32)
        outs.append(acc / total)
    o_ref[...] = jnp.concatenate(outs, axis=0).T.astype(o_ref.dtype)

def attend(query, keys, vals, other_keys, other_vals, block=512):
    tokens, width = query.shape
    kv = lambda p, b: (0, p)
    return pl.pallas_call(
        attend_kernel, grid=(width // 128, tokens // block),
        in_specs=[pl.BlockSpec((block, 128), lambda p, b: (b, p))] + [pl.BlockSpec((tokens, 128), kv)] * 4,
        out_specs=pl.BlockSpec((block, 128), lambda p, b: (b, p)),
        out_shape=jax.ShapeDtypeStruct((tokens, width), jnp.bfloat16),
        scratch_shapes=[pltpu.VMEM((128, 2 * tokens), jnp.bfloat16)],
        compiler_params=pltpu.CompilerParams(vmem_limit_bytes=60 * 1024 * 1024), name="attend",
    )(query, keys, other_keys, vals, other_vals)


def norm_rows(sums, scale, shift, count):
    channels = sums.shape[1]
    width = channels // GROUPS
    grouped = jnp.sum(sums.reshape(2, GROUPS, width), axis=-1)
    moments = (grouped + swap_cores(grouped)) / count
    mean = moments[0]
    inv_std = lax.rsqrt(moments[1] - mean * mean + NORM_EPS)
    return jnp.stack([jnp.repeat(mean, width), jnp.repeat(inv_std, width) * scale.astype(jnp.float32), shift.astype(jnp.float32)])


def channel_sums(half):
    wide = half.astype(jnp.float32)
    return jnp.stack([jnp.sum(wide, axis=(0, 1)), jnp.sum(wide * wide, axis=(0, 1))])


def edge_of(half, core):
    return jnp.where(core == 0, half[:, -1:], half[:, :1])


def attention_block(half, sums, scale, shift, w_qkv, w_out):
    rows, cols, channels = half.shape
    norm = norm_rows(sums, scale, shift, 2 * rows * cols * (channels // GROUPS))
    normed = ((half.astype(jnp.float32) - norm[0]) * norm[1] + norm[2]).astype(jnp.bfloat16).reshape(rows * cols, channels)
    flat = w_qkv.reshape(3, channels, channels)

    def project(weight):
        return jnp.dot(normed, weight, preferred_element_type=jnp.float32).astype(jnp.bfloat16)

    keys, vals = project(flat[1]), project(flat[2])
    other_keys, other_vals = swap_cores(keys), swap_cores(vals)
    query = project(flat[0])
    attended = attend(query, keys, vals, other_keys, other_vals)
    out = jnp.dot(attended, w_out.reshape(channels, channels), preferred_element_type=jnp.float32)
    return (half.astype(jnp.float32) + out.reshape(half.shape)).astype(jnp.bfloat16)


def solution(mesh):
    lat_spec = P("dp", "sp", "sp2", None)

    def local(x, time_emb, gn_scale, gn_shift, conv_w, time_w, w_qkv, w_out):
        y, core = place(lax.axis_index(SP))
        image = y * 4 + lax.axis_index(SP2)
        time_act = jax.nn.silu(time_emb.astype(jnp.float32)).astype(jnp.bfloat16)
        time_vecs = jnp.einsum("bt,stc->sbc", time_act, time_w, preferred_element_type=jnp.float32)
        time_vecs = lax.dynamic_index_in_dim(time_vecs, image, 1, keepdims=False)
        norms = gn_scale, gn_shift
        hidden, half, sums, edge = conv_in(x, gn_scale, gn_shift, time_vecs[0][None], conv_w)
        first, sums, _ = conv(hidden, swap_cores(edge), sums, swap_cores(sums), *norms, 1, conv_w, 1, half)
        middle = attention_block(first, sums, gn_scale[2], gn_shift[2], w_qkv, w_out)
        sums, edge = channel_sums(middle), edge_of(middle, core)
        hidden, sums, edge = conv(middle, swap_cores(edge), sums, swap_cores(sums), *norms, 3, conv_w, 2, time_vecs[1][None])
        return conv_out(hidden, swap_cores(edge), sums, swap_cores(sums), *norms, 4, conv_w, 3, middle)

    return jax.shard_map(local, mesh=mesh, in_specs=(lat_spec, P("dp", None), P(), P(), P(), P(), P(), P()), out_specs=lat_spec, check_vma=False)
```

```python
import functools

import jax
import jax.numpy as jnp
from jax import lax
from jax.experimental import pallas as pl
from jax.experimental.pallas import tpu as pltpu
from jax.sharding import PartitionSpec as P

GROUPS = 32
NORM_EPS = 1e-5
MESH = pl.DeviceIdType.MESH
SP, SP2 = "sp", "sp2"


def place(sp, cores=2):
    return sp // cores, lax.rem(sp, cores)


def swap_cores(value):
    return lax.ppermute(value, SP, [(0, 1), (1, 0), (2, 3), (3, 2)])


def group_rows(sums, scale, shift, count):
    channels = sums.shape[1]
    width = channels // GROUPS

    def member(shape, channel_dim):
        channel = lax.broadcasted_iota(jnp.int32, shape, channel_dim).astype(jnp.float32)
        group = lax.broadcasted_iota(jnp.int32, shape, 1 - channel_dim).astype(jnp.float32)
        return (jnp.floor((channel + 0.5) / width) == group).astype(jnp.float32)

    exact = lax.Precision.HIGHEST
    moments = jnp.dot(sums, member((channels, 128), 0), precision=exact, preferred_element_type=jnp.float32) / count
    mean = moments[0:1]
    inv_std = lax.rsqrt(moments[1:2] - mean * mean + NORM_EPS)
    spread = jnp.dot(jnp.concatenate([mean, inv_std], axis=0), member((128, channels), 1), precision=exact, preferred_element_type=jnp.float32)
    return jnp.concatenate([spread[0:1], spread[1:2] * scale.astype(jnp.float32), shift.astype(jnp.float32)], axis=0)


def silu(v):
    return v / (1.0 + jnp.exp(-v))


def fill_act(core, h_ref, other_ref, norm_ref, act):
    rows, cols, channels = h_ref.shape
    mean, mult, shift = norm_ref[0:1, :], norm_ref[1:2, :], norm_ref[2:3, :]

    def activate(v):
        return silu((v.astype(jnp.float32) - mean) * mult + shift)

    zeros = jnp.zeros((cols, channels), jnp.bfloat16)
    for dx in range(3):
        act[dx, 0] = zeros
        act[dx, rows + 1] = zeros
    line = lax.broadcasted_iota(jnp.int32, (cols, channels), 0)

    def one_row(r, carry):
        u = activate(h_ref[r])
        edge = activate(other_ref[r])
        left = jnp.where(core == 1, edge, 0.0)
        right = jnp.where(core == 0, edge, 0.0)
        act[1, r + 1] = u.astype(jnp.bfloat16)
        act[0, r + 1] = jnp.where(line == 0, left, pltpu.roll(u, 1, 0)).astype(jnp.bfloat16)
        act[2, r + 1] = jnp.where(line == cols - 1, right, pltpu.roll(u, cols - 1, 0)).astype(jnp.bfloat16)
        return carry

    lax.fori_loop(0, rows, one_row, 0)


def fetch(w_ref, wbuf, w_sem, j, n):
    width = wbuf.shape[-1]
    slot = lax.rem(n, 2)
    return pltpu.make_async_copy(w_ref.at[j, :, :, :, pl.ds(pl.multiple_of(n * width, width), width)], wbuf.at[slot], w_sem.at[slot])


def taps(act, wbuf, slot, first, rows, cols, channels):
    total = None
    for k in range(9):
        lhs = act[k % 3, pl.ds(k // 3 + first, rows)].reshape(rows * cols, channels)
        part = jnp.dot(lhs, wbuf[slot, k // 3, k % 3], preferred_element_type=jnp.float32)
        total = part if total is None else total + part
    return total


def conv_kernel(residual, norm_idx, j, h_ref, other_ref, own_ref, theirs_ref, scale_ref, shift_ref, w_ref, add_ref, out_ref, sums_ref, edge_ref, act, norm_ref, wbuf, w_sem):
    rows, cols, channels = h_ref.shape
    width = wbuf.shape[-1]
    n = pl.program_id(0)
    _, core = place(lax.axis_index(SP))

    @pl.when(n == 0)
    def _():
        fetch(w_ref, wbuf, w_sem, j, n).start()
        count = 2 * rows * cols * (channels // GROUPS)
        norm_ref[...] = group_rows(own_ref[...] + theirs_ref[...], scale_ref[norm_idx:norm_idx + 1, :], shift_ref[norm_idx:norm_idx + 1, :], count)
        fill_act(core, h_ref, other_ref, norm_ref, act)

    @pl.when(n + 1 < pl.num_programs(0))
    def _():
        fetch(w_ref, wbuf, w_sem, j, n + 1).start()

    fetch(w_ref, wbuf, w_sem, j, n).wait()
    full = taps(act, wbuf, lax.rem(n, 2), 0, rows, cols, channels)
    full = full + (add_ref[...].reshape(rows * cols, width).astype(jnp.float32) if residual else add_ref[...])
    half = full.astype(jnp.bfloat16)
    out_ref[...] = half.reshape(rows, cols, width)
    kept = half.astype(jnp.float32)
    sums_ref[...] = jnp.concatenate([jnp.sum(kept, axis=0, keepdims=True), jnp.sum(kept * kept, axis=0, keepdims=True)], axis=0)

    @pl.when(core == 0)
    def _():
        edge_ref[...] = out_ref[:, cols - 1:, :]

    @pl.when(core == 1)
    def _():
        edge_ref[...] = out_ref[:, :1, :]


def conv_specs(rows, cols, channels, nb, residual):
    whole = lambda *s: pl.BlockSpec(s, lambda n: (0,) * len(s))
    add = pl.BlockSpec((rows, cols, nb), lambda n: (0, 0, n)) if residual else pl.BlockSpec((1, nb), lambda n: (0, n))
    return [whole(rows, cols, channels), whole(rows, 1, channels), whole(2, channels), whole(2, channels), whole(5, channels), whole(5, channels), pl.BlockSpec(memory_space=pl.ANY), add]


def conv_cost(rows, cols, channels):
    return pl.CostEstimate(flops=18 * rows * cols * channels * channels, bytes_accessed=18 * channels * channels, transcendentals=rows * cols * channels)


def conv(h, other, own, theirs, scale, shift, norm_idx, w, j, add, nb=256):
    rows, cols, channels = h.shape
    return pl.pallas_call(
        functools.partial(conv_kernel, add.ndim == 3, norm_idx, j),
        grid=(channels // nb,),
        in_specs=conv_specs(rows, cols, channels, nb, add.ndim == 3),
        out_specs=[pl.BlockSpec((rows, cols, nb), lambda n: (0, 0, n)), pl.BlockSpec((2, nb), lambda n: (0, n)), pl.BlockSpec((rows, 1, nb), lambda n: (0, 0, n))],
        out_shape=[jax.ShapeDtypeStruct((rows, cols, channels), jnp.bfloat16), jax.ShapeDtypeStruct((2, channels), jnp.float32), jax.ShapeDtypeStruct((rows, 1, channels), jnp.bfloat16)],
        scratch_shapes=[pltpu.VMEM((3, rows + 2, cols, channels), jnp.bfloat16), pltpu.VMEM((3, channels), jnp.float32), pltpu.VMEM((2, 3, 3, channels, nb), jnp.bfloat16), pltpu.SemaphoreType.DMA((2,))],
        compiler_params=pltpu.CompilerParams(vmem_limit_bytes=62 * 1024 * 1024),
        cost_estimate=conv_cost(rows, cols, channels),
        name="conv",
    )(h, other, own, theirs, scale, shift, w, add)


def conv_in_kernel(x_ref, scale_ref, shift_ref, add_ref, w_ref, out_ref, half_ref, sums_ref, edge_ref,
                   tile, raw, beside, weights, act, acc, stats, heard, norm_ref,
                   tile_sem, w_sem, send_sem, recv_sem, self_sem, tell_sem, hear_sem, lend_sem, borrow_sem, keep_sem):
    images, trows, tcols, channels = x_ref.shape
    chunks, rows, cols, width = raw.shape
    sp, z = lax.axis_index(SP), lax.axis_index(SP2)
    y, core = place(sp)
    mine = y * 4 + z
    to_core = z // 2
    own = to_core == core
    me = sp * 4 + z
    load = pltpu.make_async_copy(x_ref, tile, tile_sem)
    load.start()
    barrier = pltpu.get_barrier_semaphore()
    for d in range(16):
        @pl.when(me != d)
        def _():
            pl.semaphore_signal(barrier, inc=1, device_id={SP: d // 4, SP2: d % 4}, device_id_type=MESH)

    def weight(c):
        return pltpu.make_async_copy(w_ref.at[0, :, :, pl.ds(pl.multiple_of(c * width, width), width), :], weights.at[c], w_sem.at[c])

    def lanes(c):
        return pl.ds(pl.multiple_of(c * width, width), width)

    def piece(c, src_sp, src_z):
        return raw.at[c, pl.ds(src_sp * trows, trows), pl.ds(pl.multiple_of(lax.rem(src_z, 2) * tcols, tcols), tcols), :]

    def send(c, i):
        return pltpu.make_async_remote_copy(
            src_ref=x_ref.at[i, :, :, lanes(c)], dst_ref=piece(c, sp, z), send_sem=send_sem.at[c, i], recv_sem=recv_sem.at[c, sp * 2 + lax.rem(z, 2)],
            device_id={SP: (i // 4) * 2 + to_core, SP2: i % 4}, device_id_type=MESH)

    def place_own(c):
        return pltpu.make_async_copy(x_ref.at[mine, :, :, lanes(c)], piece(c, sp, z), self_sem.at[c])

    def is_self(i):
        return own & (mine == i)

    def start_chunk(c):
        for i in range(images):
            @pl.when(jnp.logical_not(is_self(i)))
            def _():
                send(c, i).start()

        @pl.when(own)
        def _():
            place_own(c).start()

    def tell(i, k):
        return pltpu.make_async_remote_copy(
            src_ref=stats.at[i], dst_ref=heard.at[me], send_sem=tell_sem.at[i, k], recv_sem=hear_sem.at[me],
            device_id={SP: (i // 4) * 2 + k, SP2: i % 4}, device_id_type=MESH)

    pl.semaphore_wait(barrier, 15)
    start_chunk(0)
    for c in range(chunks):
        weight(c).start()
    load.wait()

    def sum_image(i, carry):
        wide = tile[i].reshape(trows * tcols, channels).astype(jnp.float32)
        stats[i] = jnp.concatenate([jnp.sum(wide, axis=0, keepdims=True), jnp.sum(wide * wide, axis=0, keepdims=True)], axis=0)
        return carry

    lax.fori_loop(0, images, sum_image, 0)
    for i in range(images):
        for k in range(2):
            @pl.when(jnp.logical_not((mine == i) & (core == k)))
            def _():
                tell(i, k).start()

    start_chunk(1)
    total = stats[mine]
    for d in range(16):
        @pl.when(me != d)
        def _():
            pltpu.make_async_remote_copy(
                src_ref=stats.at[0], dst_ref=heard.at[d], send_sem=tell_sem.at[0, 0], recv_sem=hear_sem.at[d],
                device_id={SP: d // 4, SP2: d % 4}, device_id_type=MESH).wait_recv()

        total = total + jnp.where(me != d, heard[d], 0.0)
    count = 2 * rows * cols * (channels // GROUPS)
    norm_ref[...] = group_rows(total, scale_ref[0:1, :], shift_ref[0:1, :], count)
    acc[...] = jnp.zeros_like(acc)
    zeros = jnp.zeros((cols, width), jnp.bfloat16)
    for dx in range(3):
        act[dx, 0] = zeros
        act[dx, rows + 1] = zeros
    line = lax.broadcasted_iota(jnp.int32, (cols, width), 0)
    band = beside.shape[2]

    def lend(c):
        first = pl.multiple_of((1 - core) * (cols - band), band)
        return pltpu.make_async_remote_copy(
            src_ref=raw.at[c, :, pl.ds(first, band), :], dst_ref=beside.at[c], send_sem=lend_sem.at[c], recv_sem=borrow_sem.at[c],
            device_id={SP: y * 2 + 1 - core}, device_id_type=MESH)

    def keep_raw(c):
        return pltpu.make_async_copy(raw.at[c], half_ref.at[:, :, lanes(c)], keep_sem.at[c])

    def one_chunk(c, carry):
        for s in range(8):
            src_sp, src_z = s // 2, 2 * core + s % 2

            @pl.when(jnp.logical_not((src_sp == sp) & (src_z == z)))
            def _():
                pltpu.make_async_remote_copy(
                    src_ref=x_ref.at[0, :, :, lanes(c)], dst_ref=piece(c, src_sp, src_z), send_sem=send_sem.at[c, 0], recv_sem=recv_sem.at[c, s],
                    device_id={SP: src_sp, SP2: src_z}, device_id_type=MESH).wait_recv()

        @pl.when(own)
        def _():
            place_own(c).wait()

        lend(c).start()
        keep_raw(c).start()

        @pl.when(c + 2 < chunks)
        def _():
            start_chunk(c + 2)

        mean, mult, shift = norm_ref[0:1, lanes(c)], norm_ref[1:2, lanes(c)], norm_ref[2:3, lanes(c)]

        def activate(v):
            return silu((v.astype(jnp.float32) - mean) * mult + shift)

        lend(c).wait_recv()

        def one_row(r, carry2):
            u = activate(raw[c, r])
            left = jnp.where(core == 1, activate(beside[c, r, band - 1:band, :]), 0.0)
            right = jnp.where(core == 0, activate(beside[c, r, 0:1, :]), 0.0)
            act[1, r + 1] = u.astype(jnp.bfloat16)
            act[0, r + 1] = jnp.where(line == 0, left, pltpu.roll(u, 1, 0)).astype(jnp.bfloat16)
            act[2, r + 1] = jnp.where(line == cols - 1, right, pltpu.roll(u, cols - 1, 0)).astype(jnp.bfloat16)
            return carry2

        lax.fori_loop(0, rows, one_row, 0)
        weight(c).wait()

        def one_block(n, carry2):
            part = acc[n]
            for k in range(9):
                lhs = act[k % 3, pl.ds(k // 3, rows)].reshape(rows * cols, width)
                part = part + jnp.dot(lhs, weights[c, k // 3, k % 3, :, lanes(n)], preferred_element_type=jnp.float32)
            acc[n] = part
            return carry2

        lax.fori_loop(0, chunks, one_block, 0)
        return carry

    lax.fori_loop(0, chunks, one_chunk, 0)
    for n in range(chunks):
        cut = slice(n * width, (n + 1) * width)
        half = (acc[n] + add_ref[:, cut]).astype(jnp.bfloat16)
        out_ref[:, :, cut] = half.reshape(rows, cols, width)
        kept = half.astype(jnp.float32)
        sums_ref[:, cut] = jnp.concatenate([jnp.sum(kept, axis=0, keepdims=True), jnp.sum(kept * kept, axis=0, keepdims=True)], axis=0)

    @pl.when(core == 0)
    def _():
        edge_ref[...] = out_ref[:, cols - 1:, :]

    @pl.when(core == 1)
    def _():
        edge_ref[...] = out_ref[:, :1, :]

    def drain(c, carry):
        for i in range(images):
            @pl.when(jnp.logical_not(is_self(i)))
            def _():
                send(c, i).wait_send()

        lend(c).wait_send()
        keep_raw(c).wait()
        return carry

    lax.fori_loop(0, chunks, drain, 0)
    for i in range(images):
        for k in range(2):
            @pl.when(jnp.logical_not((mine == i) & (core == k)))
            def _():
                tell(i, k).wait_send()


def conv_in(x, scale, shift, add, w, width=256, band=16):
    images, trows, tcols, channels = x.shape
    rows, cols, chunks = 4 * trows, 2 * tcols, channels // width
    vmem, hbm = pl.BlockSpec(memory_space=pltpu.VMEM), pl.BlockSpec(memory_space=pl.ANY)
    dma = pltpu.SemaphoreType.DMA
    shape = jax.ShapeDtypeStruct
    return pl.pallas_call(
        conv_in_kernel,
        in_specs=[hbm, vmem, vmem, vmem, hbm],
        out_specs=[vmem, hbm, vmem, vmem],
        out_shape=[shape((rows, cols, channels), jnp.bfloat16), shape((rows, cols, channels), jnp.bfloat16), shape((2, channels), jnp.float32), shape((rows, 1, channels), jnp.bfloat16)],
        scratch_shapes=[
            pltpu.VMEM(x.shape, jnp.bfloat16), pltpu.VMEM((chunks, rows, cols, width), jnp.bfloat16), pltpu.VMEM((chunks, rows, band, width), jnp.bfloat16),
            pltpu.VMEM((chunks, 3, 3, width, channels), jnp.bfloat16), pltpu.VMEM((3, rows + 2, cols, width), jnp.bfloat16), pltpu.VMEM((chunks, rows * cols, width), jnp.float32),
            pltpu.VMEM((images, 2, channels), jnp.float32), pltpu.VMEM((16, 2, channels), jnp.float32), pltpu.VMEM((3, channels), jnp.float32),
            dma, dma((chunks,)), dma((chunks, 8)), dma((chunks, 8)), dma((chunks,)), dma((8, 2)), dma((16,)), dma((chunks,)), dma((chunks,)), dma((chunks,))],
        compiler_params=pltpu.CompilerParams(collective_id=0, has_side_effects=True, vmem_limit_bytes=63 * 1024 * 1024),
        cost_estimate=conv_cost(rows, cols, channels),
        name="conv_in",
    )(x, scale, shift, add, w)


def conv_out_kernel(norm_idx, j, h_ref, other_ref, own_ref, theirs_ref, scale_ref, shift_ref, w_ref, add_ref, out_ref, act, norm_ref, wbuf, done, w_sem, send_sem, recv_sem, self_sem):
    rows, cols, channels = h_ref.shape
    images, trows, tcols, _ = out_ref.shape
    width = wbuf.shape[-1]
    n, chunks = pl.program_id(0), pl.num_programs(0)
    sp, z = lax.axis_index(SP), lax.axis_index(SP2)
    y, core = place(sp)
    mine = y * 4 + z
    from_core = z // 2
    own = from_core == core

    @pl.when(n == 0)
    def _():
        fetch(w_ref, wbuf, w_sem, j, n).start()
        barrier = pltpu.get_barrier_semaphore()
        for i in range(images):
            @pl.when(jnp.logical_not(own & (mine == i)))
            def _():
                pl.semaphore_signal(barrier, inc=1, device_id={SP: (i // 4) * 2 + from_core, SP2: i % 4}, device_id_type=MESH)

        count = 2 * rows * cols * (channels // GROUPS)
        norm_ref[...] = group_rows(own_ref[...] + theirs_ref[...], scale_ref[norm_idx:norm_idx + 1, :], shift_ref[norm_idx:norm_idx + 1, :], count)
        fill_act(core, h_ref, other_ref, norm_ref, act)
        pl.semaphore_wait(barrier, 8 - own.astype(jnp.int32))

    def lanes(c):
        return pl.ds(pl.multiple_of(c * width, width), width)

    def piece(c, dst_sp, dst_z):
        return done.at[c, pl.ds(dst_sp * trows, trows), pl.ds(pl.multiple_of(lax.rem(dst_z, 2) * tcols, tcols), tcols), :]

    def send(c, s):
        dst_sp, dst_z = s // 2, 2 * core + s % 2
        return pltpu.make_async_remote_copy(
            src_ref=piece(c, dst_sp, dst_z), dst_ref=out_ref.at[mine, :, :, lanes(c)], send_sem=send_sem.at[c, s], recv_sem=recv_sem.at[c, mine],
            device_id={SP: dst_sp, SP2: dst_z}, device_id_type=MESH)

    def keep(c):
        return pltpu.make_async_copy(piece(c, sp, z), out_ref.at[mine, :, :, lanes(c)], self_sem.at[c])

    def is_self(s):
        return (s // 2 == sp) & (2 * core + s % 2 == z)

    @pl.when(n + 1 < chunks)
    def _():
        fetch(w_ref, wbuf, w_sem, j, n + 1).start()

    fetch(w_ref, wbuf, w_sem, j, n).wait()
    part = rows // 2
    for m in range(2):
        span = slice(m * part, (m + 1) * part)
        full = taps(act, wbuf, lax.rem(n, 2), m * part, part, cols, channels) + add_ref[span].reshape(part * cols, width).astype(jnp.float32)
        done[n, span] = full.astype(jnp.bfloat16).reshape(part, cols, width)
        for s in range(4 * m, 4 * m + 4):
            @pl.when(jnp.logical_not(is_self(s)))
            def _():
                send(n, s).start()

    @pl.when(own)
    def _():
        keep(n).start()

    @pl.when(n == chunks - 1)
    def _():
        def drain(c, carry):
            for i in range(images):
                @pl.when(jnp.logical_not(own & (mine == i)))
                def _():
                    pltpu.make_async_remote_copy(
                        src_ref=piece(c, 0, 0), dst_ref=out_ref.at[i, :, :, lanes(c)], send_sem=send_sem.at[c, 0], recv_sem=recv_sem.at[c, i],
                        device_id={SP: (i // 4) * 2 + from_core, SP2: i % 4}, device_id_type=MESH).wait_recv()

            for s in range(8):
                @pl.when(jnp.logical_not(is_self(s)))
                def _():
                    send(c, s).wait_send()

            @pl.when(own)
            def _():
                keep(c).wait()
            return carry

        lax.fori_loop(0, channels // width, drain, 0)


def conv_out(h, other, own, theirs, scale, shift, norm_idx, w, j, add, nb=256):
    rows, cols, channels = h.shape
    chunks = channels // nb
    return pl.pallas_call(
        functools.partial(conv_out_kernel, norm_idx, j),
        grid=(chunks,),
        in_specs=conv_specs(rows, cols, channels, nb, True),
        out_specs=pl.BlockSpec(memory_space=pl.ANY),
        out_shape=jax.ShapeDtypeStruct((8, rows // 4, cols // 2, channels), jnp.bfloat16),
        scratch_shapes=[pltpu.VMEM((3, rows + 2, cols, channels), jnp.bfloat16), pltpu.VMEM((3, channels), jnp.float32), pltpu.VMEM((2, 3, 3, channels, nb), jnp.bfloat16), pltpu.VMEM((chunks, rows, cols, nb), jnp.bfloat16), pltpu.SemaphoreType.DMA((2,)),
                        pltpu.SemaphoreType.DMA((chunks, 8)), pltpu.SemaphoreType.DMA((chunks, 8)), pltpu.SemaphoreType.DMA((chunks,))],
        compiler_params=pltpu.CompilerParams(collective_id=1, has_side_effects=True, vmem_limit_bytes=62 * 1024 * 1024),
        cost_estimate=conv_cost(rows, cols, channels),
        name="conv_out",
    )(h, other, own, theirs, scale, shift, w, add)


NT = (((1,), (1,)), ((), ()))

def attend_kernel(block, chunk, q_ref, k0_ref, k1_ref, v0_ref, v1_ref, qn_ref, k0n_ref, k1n_ref, o_ref, sa, sb, peak_ref, vt):
    tokens = k0_ref.shape[0]
    pieces = 2 * tokens // chunk
    blocks = tokens // block
    items = [(b, h) for b in range(blocks) for h in range(2)]
    bufs = [sa, sb]
    lane = lax.broadcasted_iota(jnp.int32, (block, 128), 1)

    def query(ref, item):
        b, h = item
        q = ref[b * block:(b + 1) * block, :] * jnp.bfloat16(0.125)
        keep = (lane >= 64) if h else (lane < 64)
        return jnp.where(keep, q, jnp.zeros_like(q))

    def part(first, second, c):
        lo = c * chunk
        return first[lo:lo + chunk, :] if lo < tokens else second[lo - tokens:lo - tokens + chunk, :]

    def score(buf, q, first, second, c, peak):
        s = lax.dot_general(part(first, second, c), q, NT, preferred_element_type=jnp.float32)
        buf[c * chunk:(c + 1) * chunk, :] = s
        top = jnp.max(s.reshape(chunk // 8, 8, block), axis=0)
        return top if peak is None else jnp.maximum(peak, top)

    p = pl.program_id(0)

    @pl.when(p == 0)
    def _():
        q = query(q_ref, items[0])
        peak = None
        for c in range(pieces):
            peak = score(sa, q, k0_ref, k1_ref, c, peak)
        peak_ref[...] = peak

    vt[:, :tokens] = v0_ref[...].T
    vt[:, tokens:] = v1_ref[...].T
    peak8 = peak_ref[...]
    outs = []
    for t, item in enumerate(items):
        b, h = item
        cur, nxt = bufs[t % 2], bufs[(t + 1) % 2]
        last = t == len(items) - 1
        q = query(qn_ref, items[0]) if last else query(q_ref, items[t + 1])
        kf, ks = (k0n_ref, k1n_ref) if last else (k0_ref, k1_ref)
        peak = jnp.max(peak8, axis=0, keepdims=True)
        nextp, total, acc = None, None, None
        for c in range(pieces):
            nextp = score(nxt, q, kf, ks, c, nextp)
            e = jnp.exp(cur[c * chunk:(c + 1) * chunk, :] - peak)
            part_sum = jnp.sum(e.reshape(chunk // 8, 8, block), axis=0)
            total = part_sum if total is None else total + part_sum
            d = jnp.dot(vt[64 * h:64 * h + 64, c * chunk:(c + 1) * chunk], e.astype(jnp.bfloat16), preferred_element_type=jnp.float32)
            acc = d if acc is None else acc + d
        outs.append(acc / jnp.sum(total, axis=0, keepdims=True))
        peak8 = nextp
        if h == 1:
            o_ref[b * block:(b + 1) * block, :] = jnp.concatenate(outs, axis=0).T.astype(o_ref.dtype)
            outs = []
    peak_ref[...] = peak8

def attend(query, keys, vals, other_keys, other_vals, block=512, chunk=512):
    tokens, width = query.shape
    pairs = width // 128
    here = pl.BlockSpec((tokens, 128), lambda p: (0, p))
    after = pl.BlockSpec((tokens, 128), lambda p: (0, jnp.minimum(p + 1, pairs - 1)))
    return pl.pallas_call(
        functools.partial(attend_kernel, block, chunk), grid=(pairs,),
        in_specs=[here] * 5 + [after] * 3,
        out_specs=here,
        out_shape=jax.ShapeDtypeStruct((tokens, width), jnp.bfloat16),
        scratch_shapes=[pltpu.VMEM((2 * tokens, block), jnp.float32), pltpu.VMEM((2 * tokens, block), jnp.float32), pltpu.VMEM((8, block), jnp.float32), pltpu.VMEM((128, 2 * tokens), jnp.bfloat16)],
        compiler_params=pltpu.CompilerParams(vmem_limit_bytes=60 * 1024 * 1024),
        cost_estimate=pl.CostEstimate(flops=32 * tokens * tokens * width, bytes_accessed=10 * tokens * width, transcendentals=2 * tokens * tokens * width // 64),
        name="attend",
    )(query, keys, other_keys, vals, other_vals, query, keys, other_keys)


def norm_rows(sums, scale, shift, count):
    channels = sums.shape[1]
    width = channels // GROUPS
    grouped = jnp.sum(sums.reshape(2, GROUPS, width), axis=-1)
    moments = (grouped + swap_cores(grouped)) / count
    mean = moments[0]
    inv_std = lax.rsqrt(moments[1] - mean * mean + NORM_EPS)
    return jnp.stack([jnp.repeat(mean, width), jnp.repeat(inv_std, width) * scale.astype(jnp.float32), shift.astype(jnp.float32)])


def channel_sums(half):
    wide = half.astype(jnp.float32)
    return jnp.stack([jnp.sum(wide, axis=(0, 1)), jnp.sum(wide * wide, axis=(0, 1))])


def edge_of(half, core):
    return jnp.where(core == 0, half[:, -1:], half[:, :1])


def attention_block(half, sums, scale, shift, w_qkv, w_out):
    rows, cols, channels = half.shape
    norm = norm_rows(sums, scale, shift, 2 * rows * cols * (channels // GROUPS))
    normed = ((half.astype(jnp.float32) - norm[0]) * norm[1] + norm[2]).astype(jnp.bfloat16).reshape(rows * cols, channels)
    flat = w_qkv.reshape(3, channels, channels)

    def project(weight):
        return jnp.dot(normed, weight, preferred_element_type=jnp.float32).astype(jnp.bfloat16)

    keys, vals = project(flat[1]), project(flat[2])
    other_keys, other_vals = swap_cores(keys), swap_cores(vals)
    query = project(flat[0])
    attended = attend(query, keys, vals, other_keys, other_vals)
    out = jnp.dot(attended, w_out.reshape(channels, channels), preferred_element_type=jnp.float32)
    return (half.astype(jnp.float32) + out.reshape(half.shape)).astype(jnp.bfloat16)


def solution(mesh):
    lat_spec = P("dp", "sp", "sp2", None)

    def local(x, time_emb, gn_scale, gn_shift, conv_w, time_w, w_qkv, w_out):
        y, core = place(lax.axis_index(SP))
        image = y * 4 + lax.axis_index(SP2)
        time_act = jax.nn.silu(time_emb.astype(jnp.float32)).astype(jnp.bfloat16)
        time_vecs = jnp.einsum("bt,stc->sbc", time_act, time_w, preferred_element_type=jnp.float32)
        time_vecs = lax.dynamic_index_in_dim(time_vecs, image, 1, keepdims=False)
        norms = gn_scale, gn_shift
        hidden, half, sums, edge = conv_in(x, gn_scale, gn_shift, time_vecs[0][None], conv_w)
        first, sums, _ = conv(hidden, swap_cores(edge), sums, swap_cores(sums), *norms, 1, conv_w, 1, half)
        middle = attention_block(first, sums, gn_scale[2], gn_shift[2], w_qkv, w_out)
        sums, edge = channel_sums(middle), edge_of(middle, core)
        hidden, sums, edge = conv(middle, swap_cores(edge), sums, swap_cores(sums), *norms, 3, conv_w, 2, time_vecs[1][None])
        return conv_out(hidden, swap_cores(edge), sums, swap_cores(sums), *norms, 4, conv_w, 3, middle)

    return jax.shard_map(local, mesh=mesh, in_specs=(lat_spec, P("dp", None), P(), P(), P(), P(), P(), P()), out_specs=lat_spec, check_vma=False)
```

```python
import functools

import jax
import jax.numpy as jnp
from jax import lax
from jax.experimental import pallas as pl
from jax.experimental.pallas import tpu as pltpu
from jax.sharding import PartitionSpec as P

GROUPS = 32
NORM_EPS = 1e-5
MESH = pl.DeviceIdType.MESH
SP, SP2 = "sp", "sp2"


def place(sp, cores=2):
    return sp // cores, lax.rem(sp, cores)


def swap_cores(value):
    return lax.ppermute(value, SP, [(0, 1), (1, 0), (2, 3), (3, 2)])


def group_rows(sums, scale, shift, count):
    channels = sums.shape[1]
    width = channels // GROUPS

    def member(shape, channel_dim):
        channel = lax.broadcasted_iota(jnp.int32, shape, channel_dim).astype(jnp.float32)
        group = lax.broadcasted_iota(jnp.int32, shape, 1 - channel_dim).astype(jnp.float32)
        return (jnp.floor((channel + 0.5) / width) == group).astype(jnp.float32)

    exact = lax.Precision.HIGHEST
    moments = jnp.dot(sums, member((channels, 128), 0), precision=exact, preferred_element_type=jnp.float32) / count
    mean = moments[0:1]
    inv_std = lax.rsqrt(moments[1:2] - mean * mean + NORM_EPS)
    spread = jnp.dot(jnp.concatenate([mean, inv_std], axis=0), member((128, channels), 1), precision=exact, preferred_element_type=jnp.float32)
    return jnp.concatenate([spread[0:1], spread[1:2] * scale.astype(jnp.float32), shift.astype(jnp.float32)], axis=0)


def silu(v):
    return v * lax.logistic(v)


def fill_act(core, h_ref, other_ref, norm_ref, act):
    rows, cols, channels = h_ref.shape
    mean, mult, shift = norm_ref[0:1, :], norm_ref[1:2, :], norm_ref[2:3, :]

    def activate(v):
        return silu((v.astype(jnp.float32) - mean) * mult + shift)

    zeros = jnp.zeros((cols, channels), jnp.bfloat16)
    for dx in range(3):
        act[dx, 0] = zeros
        act[dx, rows + 1] = zeros
    line = lax.broadcasted_iota(jnp.int32, (cols, channels), 0)

    def one_row(r, carry):
        u = activate(h_ref[r])
        edge = activate(other_ref[r])
        left = jnp.where(core == 1, edge, 0.0)
        right = jnp.where(core == 0, edge, 0.0)
        act[1, r + 1] = u.astype(jnp.bfloat16)
        act[0, r + 1] = jnp.where(line == 0, left, pltpu.roll(u, 1, 0)).astype(jnp.bfloat16)
        act[2, r + 1] = jnp.where(line == cols - 1, right, pltpu.roll(u, cols - 1, 0)).astype(jnp.bfloat16)
        return carry

    lax.fori_loop(0, rows, one_row, 0)


def fetch(w_ref, wbuf, w_sem, j, n):
    width = wbuf.shape[-1]
    slot = lax.rem(n, 2)
    return pltpu.make_async_copy(w_ref.at[j, :, :, :, pl.ds(pl.multiple_of(n * width, width), width)], wbuf.at[slot], w_sem.at[slot])


def taps(act, wbuf, slot, first, rows, cols, channels):
    total = None
    for k in range(9):
        lhs = act[k % 3, pl.ds(k // 3 + first, rows)].reshape(rows * cols, channels)
        part = jnp.dot(lhs, wbuf[slot, k // 3, k % 3], preferred_element_type=jnp.float32)
        total = part if total is None else total + part
    return total


def conv_kernel(residual, norm_idx, j, h_ref, other_ref, own_ref, theirs_ref, scale_ref, shift_ref, w_ref, add_ref, out_ref, sums_ref, edge_ref, act, norm_ref, wbuf, w_sem):
    rows, cols, channels = h_ref.shape
    width = wbuf.shape[-1]
    n = pl.program_id(0)
    _, core = place(lax.axis_index(SP))

    @pl.when(n == 0)
    def _():
        fetch(w_ref, wbuf, w_sem, j, n).start()
        count = 2 * rows * cols * (channels // GROUPS)
        norm_ref[...] = group_rows(own_ref[...] + theirs_ref[...], scale_ref[norm_idx:norm_idx + 1, :], shift_ref[norm_idx:norm_idx + 1, :], count)
        fill_act(core, h_ref, other_ref, norm_ref, act)

    @pl.when(n + 1 < pl.num_programs(0))
    def _():
        fetch(w_ref, wbuf, w_sem, j, n + 1).start()

    fetch(w_ref, wbuf, w_sem, j, n).wait()
    full = taps(act, wbuf, lax.rem(n, 2), 0, rows, cols, channels)
    full = full + (add_ref[...].reshape(rows * cols, width).astype(jnp.float32) if residual else add_ref[...])
    half = full.astype(jnp.bfloat16)
    out_ref[...] = half.reshape(rows, cols, width)
    kept = half.astype(jnp.float32)
    sums_ref[...] = jnp.concatenate([jnp.sum(kept, axis=0, keepdims=True), jnp.sum(kept * kept, axis=0, keepdims=True)], axis=0)

    @pl.when(core == 0)
    def _():
        edge_ref[...] = out_ref[:, cols - 1:, :]

    @pl.when(core == 1)
    def _():
        edge_ref[...] = out_ref[:, :1, :]


def conv_specs(rows, cols, channels, nb, residual):
    whole = lambda *s: pl.BlockSpec(s, lambda n: (0,) * len(s))
    add = pl.BlockSpec((rows, cols, nb), lambda n: (0, 0, n)) if residual else pl.BlockSpec((1, nb), lambda n: (0, n))
    return [whole(rows, cols, channels), whole(rows, 1, channels), whole(2, channels), whole(2, channels), whole(5, channels), whole(5, channels), pl.BlockSpec(memory_space=pl.ANY), add]


def conv_cost(rows, cols, channels):
    return pl.CostEstimate(flops=18 * rows * cols * channels * channels, bytes_accessed=18 * channels * channels, transcendentals=rows * cols * channels)


def conv(h, other, own, theirs, scale, shift, norm_idx, w, j, add, nb=256):
    rows, cols, channels = h.shape
    return pl.pallas_call(
        functools.partial(conv_kernel, add.ndim == 3, norm_idx, j),
        grid=(channels // nb,),
        in_specs=conv_specs(rows, cols, channels, nb, add.ndim == 3),
        out_specs=[pl.BlockSpec((rows, cols, nb), lambda n: (0, 0, n)), pl.BlockSpec((2, nb), lambda n: (0, n)), pl.BlockSpec((rows, 1, nb), lambda n: (0, 0, n))],
        out_shape=[jax.ShapeDtypeStruct((rows, cols, channels), jnp.bfloat16), jax.ShapeDtypeStruct((2, channels), jnp.float32), jax.ShapeDtypeStruct((rows, 1, channels), jnp.bfloat16)],
        scratch_shapes=[pltpu.VMEM((3, rows + 2, cols, channels), jnp.bfloat16), pltpu.VMEM((3, channels), jnp.float32), pltpu.VMEM((2, 3, 3, channels, nb), jnp.bfloat16), pltpu.SemaphoreType.DMA((2,))],
        compiler_params=pltpu.CompilerParams(vmem_limit_bytes=62 * 1024 * 1024),
        cost_estimate=conv_cost(rows, cols, channels),
        name="conv",
    )(h, other, own, theirs, scale, shift, w, add)


def conv_in_kernel(x_ref, scale_ref, shift_ref, time_ref, tw_ref, w_ref, out_ref, half_ref, sums_ref, edge_ref, later_ref,
                   tile, raw, beside, weights, tweights, times, act, acc, stats, heard, norm_ref,
                   tile_sem, w_sem, send_sem, recv_sem, self_sem, tell_sem, hear_sem, lend_sem, borrow_sem, keep_sem, time_sem):
    images, trows, tcols, channels = x_ref.shape
    chunks, rows, cols, width = raw.shape
    sp, z = lax.axis_index(SP), lax.axis_index(SP2)
    y, core = place(sp)
    mine = y * 4 + z
    to_core = z // 2
    own = to_core == core
    me = sp * 4 + z
    load = pltpu.make_async_copy(x_ref, tile, tile_sem)
    load.start()
    barrier = pltpu.get_barrier_semaphore()
    for d in range(16):
        @pl.when(me != d)
        def _():
            pl.semaphore_signal(barrier, inc=1, device_id={SP: d // 4, SP2: d % 4}, device_id_type=MESH)

    def weight(c):
        return pltpu.make_async_copy(w_ref.at[0, :, :, pl.ds(pl.multiple_of(c * width, width), width), :], weights.at[c], w_sem.at[c])

    def lanes(c):
        return pl.ds(pl.multiple_of(c * width, width), width)

    def piece(c, src_sp, src_z):
        return raw.at[c, pl.ds(src_sp * trows, trows), pl.ds(pl.multiple_of(lax.rem(src_z, 2) * tcols, tcols), tcols), :]

    def send(c, i):
        return pltpu.make_async_remote_copy(
            src_ref=x_ref.at[i, :, :, lanes(c)], dst_ref=piece(c, sp, z), send_sem=send_sem.at[c, i], recv_sem=recv_sem.at[c, sp * 2 + lax.rem(z, 2)],
            device_id={SP: (i // 4) * 2 + to_core, SP2: lax.rem(i, 4)}, device_id_type=MESH)

    def place_own(c):
        return pltpu.make_async_copy(x_ref.at[mine, :, :, lanes(c)], piece(c, sp, z), self_sem.at[c])

    def is_self(i):
        return own & (mine == i)

    def start_chunk(c):
        for far, near in ((0, 2), (1, 3), (1, 2), (0, 3), (0, 1), (1, 1), (1, 0), (0, 0)):
            to_z = (lax.rem(z + 2, 4), 3 - z)[near - 2] if near > 1 else (z + 1 - 2 * lax.rem(z, 2) if near else z)
            i = lax.rem(y + far, 2) * 4 + to_z

            @pl.when(jnp.logical_not(is_self(i)))
            def _():
                send(c, i).start()

        @pl.when(own)
        def _():
            place_own(c).start()

    def tell(i, k):
        return pltpu.make_async_remote_copy(
            src_ref=stats.at[i], dst_ref=heard.at[me], send_sem=tell_sem.at[i, k], recv_sem=hear_sem.at[me],
            device_id={SP: (i // 4) * 2 + k, SP2: i % 4}, device_id_type=MESH)

    pl.semaphore_wait(barrier, 15)
    start_chunk(0)
    time_load = pltpu.make_async_copy(tw_ref, tweights, time_sem)
    time_load.start()
    for c in range(chunks):
        weight(c).start()
    load.wait()

    def sum_image(i, carry):
        wide = tile[i].reshape(trows * tcols, channels).astype(jnp.float32)
        stats[i] = jnp.concatenate([jnp.sum(wide, axis=0, keepdims=True), jnp.sum(wide * wide, axis=0, keepdims=True)], axis=0)
        return carry

    lax.fori_loop(0, images, sum_image, 0)
    for i in range(images):
        for k in range(2):
            @pl.when(jnp.logical_not((mine == i) & (core == k)))
            def _():
                tell(i, k).start()

    start_chunk(1)
    total = stats[mine]
    for d in range(16):
        @pl.when(me != d)
        def _():
            pltpu.make_async_remote_copy(
                src_ref=stats.at[0], dst_ref=heard.at[d], send_sem=tell_sem.at[0, 0], recv_sem=hear_sem.at[d],
                device_id={SP: d // 4, SP2: d % 4}, device_id_type=MESH).wait_recv()

        total = total + jnp.where(me != d, heard[d], 0.0)
    count = 2 * rows * cols * (channels // GROUPS)
    norm_ref[...] = group_rows(total, scale_ref[0:1, :], shift_ref[0:1, :], count)
    acc[...] = jnp.zeros_like(acc)
    time_load.wait()
    time_act = silu(time_ref[...].astype(jnp.float32)).astype(jnp.bfloat16)
    for s in range(2):
        times[s] = jnp.dot(time_act, tweights[s], preferred_element_type=jnp.float32)
    later_ref[...] = times[1, pl.ds(mine, 1), :]
    zeros = jnp.zeros((cols, width), jnp.bfloat16)
    for dx in range(3):
        act[dx, 0] = zeros
        act[dx, rows + 1] = zeros
    line = lax.broadcasted_iota(jnp.int32, (cols, width), 0)
    band = beside.shape[2]

    def lend(c):
        first = pl.multiple_of((1 - core) * (cols - band), band)
        return pltpu.make_async_remote_copy(
            src_ref=raw.at[c, :, pl.ds(first, band), :], dst_ref=beside.at[c], send_sem=lend_sem.at[c], recv_sem=borrow_sem.at[c],
            device_id={SP: y * 2 + 1 - core}, device_id_type=MESH)

    def keep_raw(c):
        return pltpu.make_async_copy(raw.at[c], half_ref.at[:, :, lanes(c)], keep_sem.at[c])

    def one_chunk(c, carry):
        for s in range(8):
            src_sp, src_z = s // 2, 2 * core + s % 2

            @pl.when(jnp.logical_not((src_sp == sp) & (src_z == z)))
            def _():
                pltpu.make_async_remote_copy(
                    src_ref=x_ref.at[0, :, :, lanes(c)], dst_ref=piece(c, src_sp, src_z), send_sem=send_sem.at[c, 0], recv_sem=recv_sem.at[c, s],
                    device_id={SP: src_sp, SP2: src_z}, device_id_type=MESH).wait_recv()

        @pl.when(own)
        def _():
            place_own(c).wait()

        lend(c).start()
        keep_raw(c).start()

        @pl.when(c + 2 < chunks)
        def _():
            start_chunk(c + 2)

        mean, mult, shift = norm_ref[0:1, lanes(c)], norm_ref[1:2, lanes(c)], norm_ref[2:3, lanes(c)]

        def activate(v):
            return silu((v.astype(jnp.float32) - mean) * mult + shift)

        lend(c).wait_recv()

        def one_row(r, carry2):
            u = activate(raw[c, r])
            left = jnp.where(core == 1, activate(beside[c, r, band - 1:band, :]), 0.0)
            right = jnp.where(core == 0, activate(beside[c, r, 0:1, :]), 0.0)
            act[1, r + 1] = u.astype(jnp.bfloat16)
            act[0, r + 1] = jnp.where(line == 0, left, pltpu.roll(u, 1, 0)).astype(jnp.bfloat16)
            act[2, r + 1] = jnp.where(line == cols - 1, right, pltpu.roll(u, cols - 1, 0)).astype(jnp.bfloat16)
            return carry2

        lax.fori_loop(0, rows, one_row, 0)
        weight(c).wait()

        def one_block(n, carry2):
            part = acc[n]
            for k in range(9):
                lhs = act[k % 3, pl.ds(k // 3, rows)].reshape(rows * cols, width)
                part = part + jnp.dot(lhs, weights[c, k // 3, k % 3, :, lanes(n)], preferred_element_type=jnp.float32)
            acc[n] = part
            return carry2

        lax.fori_loop(0, chunks, one_block, 0)
        return carry

    lax.fori_loop(0, chunks, one_chunk, 0)
    for n in range(chunks):
        cut = slice(n * width, (n + 1) * width)
        half = (acc[n] + times[0, pl.ds(mine, 1), cut]).astype(jnp.bfloat16)
        out_ref[:, :, cut] = half.reshape(rows, cols, width)
        kept = half.astype(jnp.float32)
        sums_ref[:, cut] = jnp.concatenate([jnp.sum(kept, axis=0, keepdims=True), jnp.sum(kept * kept, axis=0, keepdims=True)], axis=0)

    @pl.when(core == 0)
    def _():
        edge_ref[...] = out_ref[:, cols - 1:, :]

    @pl.when(core == 1)
    def _():
        edge_ref[...] = out_ref[:, :1, :]

    def drain(c, carry):
        for i in range(images):
            @pl.when(jnp.logical_not(is_self(i)))
            def _():
                send(c, i).wait_send()

        lend(c).wait_send()
        keep_raw(c).wait()
        return carry

    lax.fori_loop(0, chunks, drain, 0)
    for i in range(images):
        for k in range(2):
            @pl.when(jnp.logical_not((mine == i) & (core == k)))
            def _():
                tell(i, k).wait_send()


def conv_in(x, scale, shift, time_emb, time_w, w, width=256, band=16):
    images, trows, tcols, channels = x.shape
    rows, cols, chunks = 4 * trows, 2 * tcols, channels // width
    vmem, hbm = pl.BlockSpec(memory_space=pltpu.VMEM), pl.BlockSpec(memory_space=pl.ANY)
    dma = pltpu.SemaphoreType.DMA
    shape = jax.ShapeDtypeStruct
    return pl.pallas_call(
        conv_in_kernel,
        in_specs=[hbm, vmem, vmem, vmem, hbm, hbm],
        out_specs=[vmem, hbm, vmem, vmem, vmem],
        out_shape=[shape((rows, cols, channels), jnp.bfloat16), shape((rows, cols, channels), jnp.bfloat16), shape((2, channels), jnp.float32), shape((rows, 1, channels), jnp.bfloat16), shape((1, channels), jnp.float32)],
        scratch_shapes=[
            pltpu.VMEM(x.shape, jnp.bfloat16), pltpu.VMEM((chunks, rows, cols, width), jnp.bfloat16), pltpu.VMEM((chunks, rows, band, width), jnp.bfloat16),
            pltpu.VMEM((chunks, 3, 3, width, channels), jnp.bfloat16), pltpu.VMEM(time_w.shape, jnp.bfloat16), pltpu.VMEM((2, images, channels), jnp.float32), pltpu.VMEM((3, rows + 2, cols, width), jnp.bfloat16), pltpu.VMEM((chunks, rows * cols, width), jnp.float32),
            pltpu.VMEM((images, 2, channels), jnp.float32), pltpu.VMEM((16, 2, channels), jnp.float32), pltpu.VMEM((3, channels), jnp.float32),
            dma, dma((chunks,)), dma((chunks, 8)), dma((chunks, 8)), dma((chunks,)), dma((8, 2)), dma((16,)), dma((chunks,)), dma((chunks,)), dma((chunks,)), dma],
        compiler_params=pltpu.CompilerParams(collective_id=0, has_side_effects=True, vmem_limit_bytes=63 * 1024 * 1024),
        cost_estimate=conv_cost(rows, cols, channels),
        name="conv_in",
    )(x, scale, shift, time_emb, time_w, w)


def conv_out_kernel(norm_idx, j, h_ref, other_ref, own_ref, theirs_ref, scale_ref, shift_ref, w_ref, add_ref, out_ref, act, norm_ref, wbuf, done, w_sem, send_sem, recv_sem, self_sem):
    rows, cols, channels = h_ref.shape
    images, trows, tcols, _ = out_ref.shape
    width = wbuf.shape[-1]
    n, chunks = pl.program_id(0), pl.num_programs(0)
    sp, z = lax.axis_index(SP), lax.axis_index(SP2)
    y, core = place(sp)
    mine = y * 4 + z
    from_core = z // 2
    own = from_core == core

    @pl.when(n == 0)
    def _():
        fetch(w_ref, wbuf, w_sem, j, n).start()
        barrier = pltpu.get_barrier_semaphore()
        for i in range(images):
            @pl.when(jnp.logical_not(own & (mine == i)))
            def _():
                pl.semaphore_signal(barrier, inc=1, device_id={SP: (i // 4) * 2 + from_core, SP2: i % 4}, device_id_type=MESH)

        count = 2 * rows * cols * (channels // GROUPS)
        norm_ref[...] = group_rows(own_ref[...] + theirs_ref[...], scale_ref[norm_idx:norm_idx + 1, :], shift_ref[norm_idx:norm_idx + 1, :], count)
        fill_act(core, h_ref, other_ref, norm_ref, act)
        pl.semaphore_wait(barrier, 8 - own.astype(jnp.int32))

    def lanes(c):
        return pl.ds(pl.multiple_of(c * width, width), width)

    def piece(c, dst_sp, dst_z):
        return done.at[c, pl.ds(dst_sp * trows, trows), pl.ds(pl.multiple_of(lax.rem(dst_z, 2) * tcols, tcols), tcols), :]

    def send(c, s):
        dst_sp, dst_z = s // 2, 2 * core + lax.rem(s, 2)
        return pltpu.make_async_remote_copy(
            src_ref=piece(c, dst_sp, dst_z), dst_ref=out_ref.at[mine, :, :, lanes(c)], send_sem=send_sem.at[c, s], recv_sem=recv_sem.at[c, mine],
            device_id={SP: dst_sp, SP2: dst_z}, device_id_type=MESH)

    def keep(c):
        return pltpu.make_async_copy(piece(c, sp, z), out_ref.at[mine, :, :, lanes(c)], self_sem.at[c])

    def is_self(s):
        return (s // 2 == sp) & (2 * core + lax.rem(s, 2) == z)

    @pl.when(n + 1 < chunks)
    def _():
        fetch(w_ref, wbuf, w_sem, j, n + 1).start()

    fetch(w_ref, wbuf, w_sem, j, n).wait()
    full = taps(act, wbuf, lax.rem(n, 2), 0, rows, cols, channels) + add_ref[...].reshape(rows * cols, width).astype(jnp.float32)
    done[n] = full.astype(jnp.bfloat16).reshape(rows, cols, width)
    for k in range(8):
        s = (lax.rem(y + k, 2) * 2 + (k // 2) % 2) * 2 + lax.rem(z + k // 4, 2)

        @pl.when(jnp.logical_not(is_self(s)))
        def _():
            send(n, s).start()

    @pl.when(own)
    def _():
        keep(n).start()

    @pl.when(n == chunks - 1)
    def _():
        def drain(c, carry):
            for i in range(images):
                @pl.when(jnp.logical_not(own & (mine == i)))
                def _():
                    pltpu.make_async_remote_copy(
                        src_ref=piece(c, 0, 0), dst_ref=out_ref.at[i, :, :, lanes(c)], send_sem=send_sem.at[c, 0], recv_sem=recv_sem.at[c, i],
                        device_id={SP: (i // 4) * 2 + from_core, SP2: i % 4}, device_id_type=MESH).wait_recv()

            for s in range(8):
                @pl.when(jnp.logical_not(is_self(s)))
                def _():
                    send(c, s).wait_send()

            @pl.when(own)
            def _():
                keep(c).wait()
            return carry

        lax.fori_loop(0, channels // width, drain, 0)


def conv_out(h, other, own, theirs, scale, shift, norm_idx, w, j, add, nb=256):
    rows, cols, channels = h.shape
    chunks = channels // nb
    return pl.pallas_call(
        functools.partial(conv_out_kernel, norm_idx, j),
        grid=(chunks,),
        in_specs=conv_specs(rows, cols, channels, nb, True),
        out_specs=pl.BlockSpec(memory_space=pl.ANY),
        out_shape=jax.ShapeDtypeStruct((8, rows // 4, cols // 2, channels), jnp.bfloat16),
        scratch_shapes=[pltpu.VMEM((3, rows + 2, cols, channels), jnp.bfloat16), pltpu.VMEM((3, channels), jnp.float32), pltpu.VMEM((2, 3, 3, channels, nb), jnp.bfloat16), pltpu.VMEM((chunks, rows, cols, nb), jnp.bfloat16), pltpu.SemaphoreType.DMA((2,)),
                        pltpu.SemaphoreType.DMA((chunks, 8)), pltpu.SemaphoreType.DMA((chunks, 8)), pltpu.SemaphoreType.DMA((chunks,))],
        compiler_params=pltpu.CompilerParams(collective_id=1, has_side_effects=True, vmem_limit_bytes=62 * 1024 * 1024),
        cost_estimate=conv_cost(rows, cols, channels),
        name="conv_out",
    )(h, other, own, theirs, scale, shift, w, add)


NT = (((1,), (1,)), ((), ()))

def attend_kernel(block, chunk, q_ref, k0_ref, k1_ref, v0_ref, v1_ref, qn_ref, k0n_ref, k1n_ref, o_ref, sa, sb, peak_ref, vt):
    tokens = k0_ref.shape[0]
    pieces = 2 * tokens // chunk
    blocks = tokens // block
    items = [(b, h) for b in range(blocks) for h in range(2)]
    bufs = [sa, sb]
    lane = lax.broadcasted_iota(jnp.int32, (block, 128), 1)

    def query(ref, item):
        b, h = item
        q = ref[b * block:(b + 1) * block, :] * jnp.bfloat16(0.125)
        keep = (lane >= 64) if h else (lane < 64)
        return jnp.where(keep, q, jnp.zeros_like(q))

    def part(first, second, c):
        lo = c * chunk
        return first[lo:lo + chunk, :] if lo < tokens else second[lo - tokens:lo - tokens + chunk, :]

    def score(buf, q, first, second, c, peak):
        s = lax.dot_general(part(first, second, c), q, NT, preferred_element_type=jnp.float32)
        buf[c * chunk:(c + 1) * chunk, :] = s
        top = jnp.max(s.reshape(chunk // 8, 8, block), axis=0)
        return top if peak is None else jnp.maximum(peak, top)

    p = pl.program_id(0)

    @pl.when(p == 0)
    def _():
        q = query(q_ref, items[0])
        peak = None
        for c in range(pieces):
            peak = score(sa, q, k0_ref, k1_ref, c, peak)
        peak_ref[...] = peak

    vt[:, :tokens] = v0_ref[...].T
    vt[:, tokens:] = v1_ref[...].T
    peak8 = peak_ref[...]
    outs = []
    for t, item in enumerate(items):
        b, h = item
        cur, nxt = bufs[t % 2], bufs[(t + 1) % 2]
        last = t == len(items) - 1
        q = query(qn_ref, items[0]) if last else query(q_ref, items[t + 1])
        kf, ks = (k0n_ref, k1n_ref) if last else (k0_ref, k1_ref)
        peak = jnp.max(peak8, axis=0, keepdims=True)
        nextp, total, acc = None, None, None
        for c in range(pieces):
            nextp = score(nxt, q, kf, ks, c, nextp)
            e = jnp.exp(cur[c * chunk:(c + 1) * chunk, :] - peak)
            part_sum = jnp.sum(e.reshape(chunk // 8, 8, block), axis=0)
            total = part_sum if total is None else total + part_sum
            d = jnp.dot(vt[64 * h:64 * h + 64, c * chunk:(c + 1) * chunk], e.astype(jnp.bfloat16), preferred_element_type=jnp.float32)
            acc = d if acc is None else acc + d
        outs.append(acc / jnp.sum(total, axis=0, keepdims=True))
        peak8 = nextp
        if h == 1:
            o_ref[b * block:(b + 1) * block, :] = jnp.concatenate(outs, axis=0).T.astype(o_ref.dtype)
            outs = []
    peak_ref[...] = peak8

def attend(query, keys, vals, other_keys, other_vals, block=512, chunk=512):
    tokens, width = query.shape
    pairs = width // 128
    here = pl.BlockSpec((tokens, 128), lambda p: (0, p))
    after = pl.BlockSpec((tokens, 128), lambda p: (0, jnp.minimum(p + 1, pairs - 1)))
    return pl.pallas_call(
        functools.partial(attend_kernel, block, chunk), grid=(pairs,),
        in_specs=[here] * 5 + [after] * 3,
        out_specs=here,
        out_shape=jax.ShapeDtypeStruct((tokens, width), jnp.bfloat16),
        scratch_shapes=[pltpu.VMEM((2 * tokens, block), jnp.float32), pltpu.VMEM((2 * tokens, block), jnp.float32), pltpu.VMEM((8, block), jnp.float32), pltpu.VMEM((128, 2 * tokens), jnp.bfloat16)],
        compiler_params=pltpu.CompilerParams(vmem_limit_bytes=60 * 1024 * 1024),
        cost_estimate=pl.CostEstimate(flops=32 * tokens * tokens * width, bytes_accessed=10 * tokens * width, transcendentals=2 * tokens * tokens * width // 64),
        name="attend",
    )(query, keys, other_keys, vals, other_vals, query, keys, other_keys)


def norm_rows(sums, scale, shift, count):
    channels = sums.shape[1]
    width = channels // GROUPS
    grouped = jnp.sum(sums.reshape(2, GROUPS, width), axis=-1)
    moments = (grouped + swap_cores(grouped)) / count
    mean = moments[0]
    inv_std = lax.rsqrt(moments[1] - mean * mean + NORM_EPS)
    return jnp.stack([jnp.repeat(mean, width), jnp.repeat(inv_std, width) * scale.astype(jnp.float32), shift.astype(jnp.float32)])


def channel_sums(half):
    wide = half.astype(jnp.float32)
    return jnp.stack([jnp.sum(wide, axis=(0, 1)), jnp.sum(wide * wide, axis=(0, 1))])


def edge_of(half, core):
    return jnp.where(core == 0, half[:, -1:], half[:, :1])


def attention_block(half, sums, scale, shift, w_qkv, w_out):
    rows, cols, channels = half.shape
    norm = norm_rows(sums, scale, shift, 2 * rows * cols * (channels // GROUPS))
    normed = ((half.astype(jnp.float32) - norm[0]) * norm[1] + norm[2]).astype(jnp.bfloat16).reshape(rows * cols, channels)
    flat = w_qkv.reshape(3, channels, channels)

    def project(weight):
        return jnp.dot(normed, weight, preferred_element_type=jnp.float32).astype(jnp.bfloat16)

    keys, vals = project(flat[1]), project(flat[2])
    other_keys, other_vals = swap_cores(keys), swap_cores(vals)
    query = project(flat[0])
    attended = attend(query, keys, vals, other_keys, other_vals)
    out = jnp.dot(attended, w_out.reshape(channels, channels), preferred_element_type=jnp.float32)
    return (half.astype(jnp.float32) + out.reshape(half.shape)).astype(jnp.bfloat16)


def solution(mesh):
    lat_spec = P("dp", "sp", "sp2", None)

    def local(x, time_emb, gn_scale, gn_shift, conv_w, time_w, w_qkv, w_out):
        _, core = place(lax.axis_index(SP))
        norms = gn_scale, gn_shift
        hidden, half, sums, edge, time_vec = conv_in(x, gn_scale, gn_shift, time_emb, time_w, conv_w)
        first, sums, _ = conv(hidden, swap_cores(edge), sums, swap_cores(sums), *norms, 1, conv_w, 1, half)
        middle = attention_block(first, sums, gn_scale[2], gn_shift[2], w_qkv, w_out)
        sums, edge = channel_sums(middle), edge_of(middle, core)
        hidden, sums, edge = conv(middle, swap_cores(edge), sums, swap_cores(sums), *norms, 3, conv_w, 2, time_vec)
        return conv_out(hidden, swap_cores(edge), sums, swap_cores(sums), *norms, 4, conv_w, 3, middle)

    return jax.shard_map(local, mesh=mesh, in_specs=(lat_spec, P("dp", None), P(), P(), P(), P(), P(), P()), out_specs=lat_spec, check_vma=False)
```

```python
import functools

import jax
import jax.numpy as jnp
from jax import lax
from jax.experimental import pallas as pl
from jax.experimental.pallas import tpu as pltpu
from jax.sharding import PartitionSpec as P

GROUPS = 32
NORM_EPS = 1e-5
MESH = pl.DeviceIdType.MESH
SP, SP2 = "sp", "sp2"


def place(sp, cores=2):
    return sp // cores, lax.rem(sp, cores)


def swap_cores(value):
    return lax.ppermute(value, SP, [(0, 1), (1, 0), (2, 3), (3, 2)])


def group_rows(sums, scale, shift, count):
    channels = sums.shape[1]
    width = channels // GROUPS

    def member(shape, channel_dim):
        channel = lax.broadcasted_iota(jnp.int32, shape, channel_dim).astype(jnp.float32)
        group = lax.broadcasted_iota(jnp.int32, shape, 1 - channel_dim).astype(jnp.float32)
        return (jnp.floor((channel + 0.5) / width) == group).astype(jnp.float32)

    exact = lax.Precision.HIGHEST
    moments = jnp.dot(sums, member((channels, 128), 0), precision=exact, preferred_element_type=jnp.float32) / count
    mean = moments[0:1]
    inv_std = lax.rsqrt(moments[1:2] - mean * mean + NORM_EPS)
    spread = jnp.dot(jnp.concatenate([mean, inv_std], axis=0), member((128, channels), 1), precision=exact, preferred_element_type=jnp.float32)
    return jnp.concatenate([spread[0:1], spread[1:2] * scale.astype(jnp.float32), shift.astype(jnp.float32)], axis=0)


def silu(v):
    return v * lax.logistic(v)


def fill_act(core, h_ref, other_ref, norm_ref, act):
    rows, cols, channels = h_ref.shape
    mean, mult, shift = norm_ref[0:1, :], norm_ref[1:2, :], norm_ref[2:3, :]

    def activate(v):
        return silu((v.astype(jnp.float32) - mean) * mult + shift)

    zeros = jnp.zeros((cols, channels), jnp.bfloat16)
    for dx in range(3):
        act[dx, 0] = zeros
        act[dx, rows + 1] = zeros
    line = lax.broadcasted_iota(jnp.int32, (cols, channels), 0)

    def one_row(r, carry):
        u = activate(h_ref[r])
        edge = activate(other_ref[r])
        left = jnp.where(core == 1, edge, 0.0)
        right = jnp.where(core == 0, edge, 0.0)
        act[1, r + 1] = u.astype(jnp.bfloat16)
        act[0, r + 1] = jnp.where(line == 0, left, pltpu.roll(u, 1, 0)).astype(jnp.bfloat16)
        act[2, r + 1] = jnp.where(line == cols - 1, right, pltpu.roll(u, cols - 1, 0)).astype(jnp.bfloat16)
        return carry

    lax.fori_loop(0, rows, one_row, 0)


def fetch(w_ref, wbuf, w_sem, j, n):
    width = wbuf.shape[-1]
    slot = lax.rem(n, 2)
    return pltpu.make_async_copy(w_ref.at[j, :, :, :, pl.ds(pl.multiple_of(n * width, width), width)], wbuf.at[slot], w_sem.at[slot])


def taps(act, wbuf, slot, first, rows, cols, channels):
    total = None
    for k in range(9):
        lhs = act[k % 3, pl.ds(k // 3 + first, rows)].reshape(rows * cols, channels)
        part = jnp.dot(lhs, wbuf[slot, k // 3, k % 3], preferred_element_type=jnp.float32)
        total = part if total is None else total + part
    return total


def conv_kernel(residual, norm_idx, j, h_ref, other_ref, own_ref, theirs_ref, scale_ref, shift_ref, w_ref, add_ref, out_ref, sums_ref, edge_ref, act, norm_ref, wbuf, w_sem):
    rows, cols, channels = h_ref.shape
    width = wbuf.shape[-1]
    n = pl.program_id(0)
    _, core = place(lax.axis_index(SP))

    @pl.when(n == 0)
    def _():
        fetch(w_ref, wbuf, w_sem, j, n).start()
        count = 2 * rows * cols * (channels // GROUPS)
        norm_ref[...] = group_rows(own_ref[...] + theirs_ref[...], scale_ref[norm_idx:norm_idx + 1, :], shift_ref[norm_idx:norm_idx + 1, :], count)
        fill_act(core, h_ref, other_ref, norm_ref, act)

    @pl.when(n + 1 < pl.num_programs(0))
    def _():
        fetch(w_ref, wbuf, w_sem, j, n + 1).start()

    fetch(w_ref, wbuf, w_sem, j, n).wait()
    full = taps(act, wbuf, lax.rem(n, 2), 0, rows, cols, channels)
    full = full + (add_ref[...].reshape(rows * cols, width).astype(jnp.float32) if residual else add_ref[...])
    half = full.astype(jnp.bfloat16)
    out_ref[...] = half.reshape(rows, cols, width)
    kept = half.astype(jnp.float32)
    sums_ref[...] = jnp.concatenate([jnp.sum(kept, axis=0, keepdims=True), jnp.sum(kept * kept, axis=0, keepdims=True)], axis=0)

    @pl.when(core == 0)
    def _():
        edge_ref[...] = out_ref[:, cols - 1:, :]

    @pl.when(core == 1)
    def _():
        edge_ref[...] = out_ref[:, :1, :]


def conv_specs(rows, cols, channels, nb, residual):
    whole = lambda *s: pl.BlockSpec(s, lambda n: (0,) * len(s))
    add = pl.BlockSpec((rows, cols, nb), lambda n: (0, 0, n)) if residual else pl.BlockSpec((1, nb), lambda n: (0, n))
    return [whole(rows, cols, channels), whole(rows, 1, channels), whole(2, channels), whole(2, channels), whole(5, channels), whole(5, channels), pl.BlockSpec(memory_space=pl.ANY), add]


def conv_cost(rows, cols, channels):
    return pl.CostEstimate(flops=18 * rows * cols * channels * channels, bytes_accessed=18 * channels * channels, transcendentals=rows * cols * channels)


def conv(h, other, own, theirs, scale, shift, norm_idx, w, j, add, nb=256):
    rows, cols, channels = h.shape
    return pl.pallas_call(
        functools.partial(conv_kernel, add.ndim == 3, norm_idx, j),
        grid=(channels // nb,),
        in_specs=conv_specs(rows, cols, channels, nb, add.ndim == 3),
        out_specs=[pl.BlockSpec((rows, cols, nb), lambda n: (0, 0, n)), pl.BlockSpec((2, nb), lambda n: (0, n)), pl.BlockSpec((rows, 1, nb), lambda n: (0, 0, n))],
        out_shape=[jax.ShapeDtypeStruct((rows, cols, channels), jnp.bfloat16), jax.ShapeDtypeStruct((2, channels), jnp.float32), jax.ShapeDtypeStruct((rows, 1, channels), jnp.bfloat16)],
        scratch_shapes=[pltpu.VMEM((3, rows + 2, cols, channels), jnp.bfloat16), pltpu.VMEM((3, channels), jnp.float32), pltpu.VMEM((2, 3, 3, channels, nb), jnp.bfloat16), pltpu.SemaphoreType.DMA((2,))],
        compiler_params=pltpu.CompilerParams(vmem_limit_bytes=62 * 1024 * 1024),
        cost_estimate=conv_cost(rows, cols, channels),
        name="conv",
    )(h, other, own, theirs, scale, shift, w, add)


def conv_in_kernel(x_ref, scale_ref, shift_ref, time_ref, tw_ref, w_ref, out_ref, half_ref, sums_ref, edge_ref, later_ref,
                   tile, raw, beside, weights, tweights, times, act, acc, stats, heard, norm_ref,
                   tile_sem, w_sem, send_sem, recv_sem, self_sem, tell_sem, hear_sem, lend_sem, borrow_sem, keep_sem, time_sem):
    images, trows, tcols, channels = x_ref.shape
    chunks, rows, cols, width = raw.shape
    sp, z = lax.axis_index(SP), lax.axis_index(SP2)
    y, core = place(sp)
    mine = y * 4 + z
    to_core = z // 2
    own = to_core == core
    me = sp * 4 + z
    load = pltpu.make_async_copy(x_ref, tile, tile_sem)
    load.start()
    barrier = pltpu.get_barrier_semaphore()
    for d in range(16):
        @pl.when(me != d)
        def _():
            pl.semaphore_signal(barrier, inc=1, device_id={SP: d // 4, SP2: d % 4}, device_id_type=MESH)

    def weight(c):
        return pltpu.make_async_copy(w_ref.at[0, :, :, pl.ds(pl.multiple_of(c * width, width), width), :], weights.at[c], w_sem.at[c])

    def lanes(c):
        return pl.ds(pl.multiple_of(c * width, width), width)

    def piece(c, src_sp, src_z):
        return raw.at[c, pl.ds(src_sp * trows, trows), pl.ds(pl.multiple_of(lax.rem(src_z, 2) * tcols, tcols), tcols), :]

    def send(c, i):
        return pltpu.make_async_remote_copy(
            src_ref=tile.at[i, :, :, lanes(c)], dst_ref=piece(c, sp, z), send_sem=send_sem.at[c, i], recv_sem=recv_sem.at[c, sp * 2 + lax.rem(z, 2)],
            device_id={SP: (i // 4) * 2 + to_core, SP2: lax.rem(i, 4)}, device_id_type=MESH)

    def place_own(c):
        return pltpu.make_async_copy(x_ref.at[mine, :, :, lanes(c)], piece(c, sp, z), self_sem.at[c])

    def is_self(i):
        return own & (mine == i)

    def start_chunk(c):
        for far, near in ((0, 2), (1, 3), (1, 2), (0, 3), (0, 1), (1, 1), (1, 0), (0, 0)):
            to_z = (lax.rem(z + 2, 4), 3 - z)[near - 2] if near > 1 else (z + 1 - 2 * lax.rem(z, 2) if near else z)
            i = lax.rem(y + far, 2) * 4 + to_z

            @pl.when(jnp.logical_not(is_self(i)))
            def _():
                send(c, i).start()

        @pl.when(own)
        def _():
            place_own(c).start()

    def tell(i, k):
        return pltpu.make_async_remote_copy(
            src_ref=stats.at[i], dst_ref=heard.at[me], send_sem=tell_sem.at[i, k], recv_sem=hear_sem.at[me],
            device_id={SP: (i // 4) * 2 + k, SP2: i % 4}, device_id_type=MESH)

    load.wait()
    pl.semaphore_wait(barrier, 15)
    start_chunk(0)
    time_load = pltpu.make_async_copy(tw_ref, tweights, time_sem)
    time_load.start()
    for c in range(chunks):
        weight(c).start()

    def sum_image(i, carry):
        wide = tile[i].reshape(trows * tcols, channels).astype(jnp.float32)
        stats[i] = jnp.concatenate([jnp.sum(wide, axis=0, keepdims=True), jnp.sum(wide * wide, axis=0, keepdims=True)], axis=0)
        return carry

    lax.fori_loop(0, images, sum_image, 0)
    for i in range(images):
        for k in range(2):
            @pl.when(jnp.logical_not((mine == i) & (core == k)))
            def _():
                tell(i, k).start()

    start_chunk(1)
    total = stats[mine]
    for d in range(16):
        @pl.when(me != d)
        def _():
            pltpu.make_async_remote_copy(
                src_ref=stats.at[0], dst_ref=heard.at[d], send_sem=tell_sem.at[0, 0], recv_sem=hear_sem.at[d],
                device_id={SP: d // 4, SP2: d % 4}, device_id_type=MESH).wait_recv()

        total = total + jnp.where(me != d, heard[d], 0.0)
    count = 2 * rows * cols * (channels // GROUPS)
    norm_ref[...] = group_rows(total, scale_ref[0:1, :], shift_ref[0:1, :], count)
    acc[...] = jnp.zeros_like(acc)
    time_load.wait()
    time_act = silu(time_ref[...].astype(jnp.float32)).astype(jnp.bfloat16)
    for s in range(2):
        times[s] = jnp.dot(time_act, tweights[s], preferred_element_type=jnp.float32)
    later_ref[...] = times[1, pl.ds(mine, 1), :]
    zeros = jnp.zeros((cols, width), jnp.bfloat16)
    for dx in range(3):
        act[dx, 0] = zeros
        act[dx, rows + 1] = zeros
    line = lax.broadcasted_iota(jnp.int32, (cols, width), 0)
    band = beside.shape[2]

    def lend(c):
        first = pl.multiple_of((1 - core) * (cols - band), band)
        return pltpu.make_async_remote_copy(
            src_ref=raw.at[c, :, pl.ds(first, band), :], dst_ref=beside.at[c], send_sem=lend_sem.at[c], recv_sem=borrow_sem.at[c],
            device_id={SP: y * 2 + 1 - core}, device_id_type=MESH)

    def keep_raw(c):
        return pltpu.make_async_copy(raw.at[c], half_ref.at[:, :, lanes(c)], keep_sem.at[c])

    def one_chunk(c, carry):
        for s in range(8):
            src_sp, src_z = s // 2, 2 * core + s % 2

            @pl.when(jnp.logical_not((src_sp == sp) & (src_z == z)))
            def _():
                pltpu.make_async_remote_copy(
                    src_ref=x_ref.at[0, :, :, lanes(c)], dst_ref=piece(c, src_sp, src_z), send_sem=send_sem.at[c, 0], recv_sem=recv_sem.at[c, s],
                    device_id={SP: src_sp, SP2: src_z}, device_id_type=MESH).wait_recv()

        @pl.when(own)
        def _():
            place_own(c).wait()

        lend(c).start()
        keep_raw(c).start()

        @pl.when(c + 2 < chunks)
        def _():
            start_chunk(c + 2)

        mean, mult, shift = norm_ref[0:1, lanes(c)], norm_ref[1:2, lanes(c)], norm_ref[2:3, lanes(c)]

        def activate(v):
            return silu((v.astype(jnp.float32) - mean) * mult + shift)

        lend(c).wait_recv()

        def one_row(r, carry2):
            u = activate(raw[c, r])
            left = jnp.where(core == 1, activate(beside[c, r, band - 1:band, :]), 0.0)
            right = jnp.where(core == 0, activate(beside[c, r, 0:1, :]), 0.0)
            act[1, r + 1] = u.astype(jnp.bfloat16)
            act[0, r + 1] = jnp.where(line == 0, left, pltpu.roll(u, 1, 0)).astype(jnp.bfloat16)
            act[2, r + 1] = jnp.where(line == cols - 1, right, pltpu.roll(u, cols - 1, 0)).astype(jnp.bfloat16)
            return carry2

        lax.fori_loop(0, rows, one_row, 0)
        weight(c).wait()

        def one_block(n, carry2):
            part = acc[n]
            for k in range(9):
                lhs = act[k % 3, pl.ds(k // 3, rows)].reshape(rows * cols, width)
                part = part + jnp.dot(lhs, weights[c, k // 3, k % 3, :, lanes(n)], preferred_element_type=jnp.float32)
            acc[n] = part
            return carry2

        lax.fori_loop(0, chunks, one_block, 0)
        return carry

    lax.fori_loop(0, chunks, one_chunk, 0)
    for n in range(chunks):
        cut = slice(n * width, (n + 1) * width)
        half = (acc[n] + times[0, pl.ds(mine, 1), cut]).astype(jnp.bfloat16)
        out_ref[:, :, cut] = half.reshape(rows, cols, width)
        kept = half.astype(jnp.float32)
        sums_ref[:, cut] = jnp.concatenate([jnp.sum(kept, axis=0, keepdims=True), jnp.sum(kept * kept, axis=0, keepdims=True)], axis=0)

    @pl.when(core == 0)
    def _():
        edge_ref[...] = out_ref[:, cols - 1:, :]

    @pl.when(core == 1)
    def _():
        edge_ref[...] = out_ref[:, :1, :]

    def drain(c, carry):
        for i in range(images):
            @pl.when(jnp.logical_not(is_self(i)))
            def _():
                send(c, i).wait_send()

        lend(c).wait_send()
        keep_raw(c).wait()
        return carry

    lax.fori_loop(0, chunks, drain, 0)
    for i in range(images):
        for k in range(2):
            @pl.when(jnp.logical_not((mine == i) & (core == k)))
            def _():
                tell(i, k).wait_send()


def conv_in(x, scale, shift, time_emb, time_w, w, width=256, band=16):
    images, trows, tcols, channels = x.shape
    rows, cols, chunks = 4 * trows, 2 * tcols, channels // width
    vmem, hbm = pl.BlockSpec(memory_space=pltpu.VMEM), pl.BlockSpec(memory_space=pl.ANY)
    dma = pltpu.SemaphoreType.DMA
    shape = jax.ShapeDtypeStruct
    return pl.pallas_call(
        conv_in_kernel,
        in_specs=[hbm, vmem, vmem, vmem, hbm, hbm],
        out_specs=[vmem, hbm, vmem, vmem, vmem],
        out_shape=[shape((rows, cols, channels), jnp.bfloat16), shape((rows, cols, channels), jnp.bfloat16), shape((2, channels), jnp.float32), shape((rows, 1, channels), jnp.bfloat16), shape((1, channels), jnp.float32)],
        scratch_shapes=[
            pltpu.VMEM(x.shape, jnp.bfloat16), pltpu.VMEM((chunks, rows, cols, width), jnp.bfloat16), pltpu.VMEM((chunks, rows, band, width), jnp.bfloat16),
            pltpu.VMEM((chunks, 3, 3, width, channels), jnp.bfloat16), pltpu.VMEM(time_w.shape, jnp.bfloat16), pltpu.VMEM((2, images, channels), jnp.float32), pltpu.VMEM((3, rows + 2, cols, width), jnp.bfloat16), pltpu.VMEM((chunks, rows * cols, width), jnp.float32),
            pltpu.VMEM((images, 2, channels), jnp.float32), pltpu.VMEM((16, 2, channels), jnp.float32), pltpu.VMEM((3, channels), jnp.float32),
            dma, dma((chunks,)), dma((chunks, 8)), dma((chunks, 8)), dma((chunks,)), dma((8, 2)), dma((16,)), dma((chunks,)), dma((chunks,)), dma((chunks,)), dma],
        compiler_params=pltpu.CompilerParams(collective_id=0, has_side_effects=True, vmem_limit_bytes=63 * 1024 * 1024),
        cost_estimate=conv_cost(rows, cols, channels),
        name="conv_in",
    )(x, scale, shift, time_emb, time_w, w)


def conv_out_kernel(norm_idx, j, h_ref, other_ref, own_ref, theirs_ref, scale_ref, shift_ref, w_ref, add_ref, out_ref, act, norm_ref, wbuf, done, w_sem, send_sem, recv_sem, self_sem):
    rows, cols, channels = h_ref.shape
    images, trows, tcols, _ = out_ref.shape
    width = wbuf.shape[-1]
    n, chunks = pl.program_id(0), pl.num_programs(0)
    sp, z = lax.axis_index(SP), lax.axis_index(SP2)
    y, core = place(sp)
    mine = y * 4 + z
    from_core = z // 2
    own = from_core == core

    @pl.when(n == 0)
    def _():
        fetch(w_ref, wbuf, w_sem, j, n).start()
        barrier = pltpu.get_barrier_semaphore()
        for i in range(images):
            @pl.when(jnp.logical_not(own & (mine == i)))
            def _():
                pl.semaphore_signal(barrier, inc=1, device_id={SP: (i // 4) * 2 + from_core, SP2: i % 4}, device_id_type=MESH)

        count = 2 * rows * cols * (channels // GROUPS)
        norm_ref[...] = group_rows(own_ref[...] + theirs_ref[...], scale_ref[norm_idx:norm_idx + 1, :], shift_ref[norm_idx:norm_idx + 1, :], count)
        fill_act(core, h_ref, other_ref, norm_ref, act)
        pl.semaphore_wait(barrier, 8 - own.astype(jnp.int32))

    def lanes(c):
        return pl.ds(pl.multiple_of(c * width, width), width)

    def piece(c, dst_sp, dst_z):
        return done.at[c, pl.ds(dst_sp * trows, trows), pl.ds(pl.multiple_of(lax.rem(dst_z, 2) * tcols, tcols), tcols), :]

    def send(c, s):
        dst_sp, dst_z = s // 2, 2 * core + lax.rem(s, 2)
        return pltpu.make_async_remote_copy(
            src_ref=piece(c, dst_sp, dst_z), dst_ref=out_ref.at[mine, :, :, lanes(c)], send_sem=send_sem.at[c, s], recv_sem=recv_sem.at[c, mine],
            device_id={SP: dst_sp, SP2: dst_z}, device_id_type=MESH)

    def keep(c):
        return pltpu.make_async_copy(piece(c, sp, z), out_ref.at[mine, :, :, lanes(c)], self_sem.at[c])

    def is_self(s):
        return (s // 2 == sp) & (2 * core + lax.rem(s, 2) == z)

    @pl.when(n + 1 < chunks)
    def _():
        fetch(w_ref, wbuf, w_sem, j, n + 1).start()

    fetch(w_ref, wbuf, w_sem, j, n).wait()
    full = taps(act, wbuf, lax.rem(n, 2), 0, rows, cols, channels) + add_ref[...].reshape(rows * cols, width).astype(jnp.float32)
    done[n] = full.astype(jnp.bfloat16).reshape(rows, cols, width)
    for k in range(8):
        s = (lax.rem(y + k, 2) * 2 + (k // 2) % 2) * 2 + lax.rem(z + k // 4, 2)

        @pl.when(jnp.logical_not(is_self(s)))
        def _():
            send(n, s).start()

    @pl.when(own)
    def _():
        keep(n).start()

    @pl.when(n == chunks - 1)
    def _():
        def drain(c, carry):
            for i in range(images):
                @pl.when(jnp.logical_not(own & (mine == i)))
                def _():
                    pltpu.make_async_remote_copy(
                        src_ref=piece(c, 0, 0), dst_ref=out_ref.at[i, :, :, lanes(c)], send_sem=send_sem.at[c, 0], recv_sem=recv_sem.at[c, i],
                        device_id={SP: (i // 4) * 2 + from_core, SP2: i % 4}, device_id_type=MESH).wait_recv()

            for s in range(8):
                @pl.when(jnp.logical_not(is_self(s)))
                def _():
                    send(c, s).wait_send()

            @pl.when(own)
            def _():
                keep(c).wait()
            return carry

        lax.fori_loop(0, channels // width, drain, 0)


def conv_out(h, other, own, theirs, scale, shift, norm_idx, w, j, add, nb=256):
    rows, cols, channels = h.shape
    chunks = channels // nb
    return pl.pallas_call(
        functools.partial(conv_out_kernel, norm_idx, j),
        grid=(chunks,),
        in_specs=conv_specs(rows, cols, channels, nb, True),
        out_specs=pl.BlockSpec(memory_space=pl.ANY),
        out_shape=jax.ShapeDtypeStruct((8, rows // 4, cols // 2, channels), jnp.bfloat16),
        scratch_shapes=[pltpu.VMEM((3, rows + 2, cols, channels), jnp.bfloat16), pltpu.VMEM((3, channels), jnp.float32), pltpu.VMEM((2, 3, 3, channels, nb), jnp.bfloat16), pltpu.VMEM((chunks, rows, cols, nb), jnp.bfloat16), pltpu.SemaphoreType.DMA((2,)),
                        pltpu.SemaphoreType.DMA((chunks, 8)), pltpu.SemaphoreType.DMA((chunks, 8)), pltpu.SemaphoreType.DMA((chunks,))],
        compiler_params=pltpu.CompilerParams(collective_id=1, has_side_effects=True, vmem_limit_bytes=62 * 1024 * 1024),
        cost_estimate=conv_cost(rows, cols, channels),
        name="conv_out",
    )(h, other, own, theirs, scale, shift, w, add)


NT = (((1,), (1,)), ((), ()))

def attend_kernel(block, chunk, q_ref, k0_ref, k1_ref, v0_ref, v1_ref, qn_ref, k0n_ref, k1n_ref, o_ref, sa, sb, peak_ref, vt):
    tokens = k0_ref.shape[0]
    pieces = 2 * tokens // chunk
    blocks = tokens // block
    items = [(b, h) for b in range(blocks) for h in range(2)]
    bufs = [sa, sb]
    lane = lax.broadcasted_iota(jnp.int32, (block, 128), 1)

    def query(ref, item):
        b, h = item
        q = ref[b * block:(b + 1) * block, :] * jnp.bfloat16(0.125)
        keep = (lane >= 64) if h else (lane < 64)
        return jnp.where(keep, q, jnp.zeros_like(q))

    def part(first, second, c):
        lo = c * chunk
        return first[lo:lo + chunk, :] if lo < tokens else second[lo - tokens:lo - tokens + chunk, :]

    def score(buf, q, first, second, c, peak):
        s = lax.dot_general(part(first, second, c), q, NT, preferred_element_type=jnp.float32)
        buf[c * chunk:(c + 1) * chunk, :] = s
        top = jnp.max(s.reshape(chunk // 8, 8, block), axis=0)
        return top if peak is None else jnp.maximum(peak, top)

    p = pl.program_id(0)

    @pl.when(p == 0)
    def _():
        q = query(q_ref, items[0])
        peak = None
        for c in range(pieces):
            peak = score(sa, q, k0_ref, k1_ref, c, peak)
        peak_ref[...] = peak

    vt[:, :tokens] = v0_ref[...].T
    vt[:, tokens:] = v1_ref[...].T
    peak8 = peak_ref[...]
    outs = []
    for t, item in enumerate(items):
        b, h = item
        cur, nxt = bufs[t % 2], bufs[(t + 1) % 2]
        last = t == len(items) - 1
        q = query(qn_ref, items[0]) if last else query(q_ref, items[t + 1])
        kf, ks = (k0n_ref, k1n_ref) if last else (k0_ref, k1_ref)
        peak = jnp.max(peak8, axis=0, keepdims=True)
        nextp, total, acc = None, None, None
        for c in range(pieces):
            nextp = score(nxt, q, kf, ks, c, nextp)
            e = jnp.exp(cur[c * chunk:(c + 1) * chunk, :] - peak)
            part_sum = jnp.sum(e.reshape(chunk // 8, 8, block), axis=0)
            total = part_sum if total is None else total + part_sum
            d = jnp.dot(vt[64 * h:64 * h + 64, c * chunk:(c + 1) * chunk], e.astype(jnp.bfloat16), preferred_element_type=jnp.float32)
            acc = d if acc is None else acc + d
        outs.append(acc / jnp.sum(total, axis=0, keepdims=True))
        peak8 = nextp
        if h == 1:
            o_ref[b * block:(b + 1) * block, :] = jnp.concatenate(outs, axis=0).T.astype(o_ref.dtype)
            outs = []
    peak_ref[...] = peak8

def attend(query, keys, vals, other_keys, other_vals, block=512, chunk=512):
    tokens, width = query.shape
    pairs = width // 128
    here = pl.BlockSpec((tokens, 128), lambda p: (0, p))
    after = pl.BlockSpec((tokens, 128), lambda p: (0, jnp.minimum(p + 1, pairs - 1)))
    return pl.pallas_call(
        functools.partial(attend_kernel, block, chunk), grid=(pairs,),
        in_specs=[here] * 5 + [after] * 3,
        out_specs=here,
        out_shape=jax.ShapeDtypeStruct((tokens, width), jnp.bfloat16),
        scratch_shapes=[pltpu.VMEM((2 * tokens, block), jnp.float32), pltpu.VMEM((2 * tokens, block), jnp.float32), pltpu.VMEM((8, block), jnp.float32), pltpu.VMEM((128, 2 * tokens), jnp.bfloat16)],
        compiler_params=pltpu.CompilerParams(vmem_limit_bytes=60 * 1024 * 1024),
        cost_estimate=pl.CostEstimate(flops=32 * tokens * tokens * width, bytes_accessed=10 * tokens * width, transcendentals=2 * tokens * tokens * width // 64),
        name="attend",
    )(query, keys, other_keys, vals, other_vals, query, keys, other_keys)


def norm_rows(sums, scale, shift, count):
    channels = sums.shape[1]
    width = channels // GROUPS
    grouped = jnp.sum(sums.reshape(2, GROUPS, width), axis=-1)
    moments = (grouped + swap_cores(grouped)) / count
    mean = moments[0]
    inv_std = lax.rsqrt(moments[1] - mean * mean + NORM_EPS)
    return jnp.stack([jnp.repeat(mean, width), jnp.repeat(inv_std, width) * scale.astype(jnp.float32), shift.astype(jnp.float32)])


def channel_sums(half):
    wide = half.astype(jnp.float32)
    return jnp.stack([jnp.sum(wide, axis=(0, 1)), jnp.sum(wide * wide, axis=(0, 1))])


def edge_of(half, core):
    return jnp.where(core == 0, half[:, -1:], half[:, :1])


def attention_block(half, sums, scale, shift, w_qkv, w_out):
    rows, cols, channels = half.shape
    norm = norm_rows(sums, scale, shift, 2 * rows * cols * (channels // GROUPS))
    normed = ((half.astype(jnp.float32) - norm[0]) * norm[1] + norm[2]).astype(jnp.bfloat16).reshape(rows * cols, channels)
    flat = w_qkv.reshape(3, channels, channels)

    def project(weight):
        return jnp.dot(normed, weight, preferred_element_type=jnp.float32).astype(jnp.bfloat16)

    keys, vals = project(flat[1]), project(flat[2])
    other_keys, other_vals = swap_cores(keys), swap_cores(vals)
    query = project(flat[0])
    attended = attend(query, keys, vals, other_keys, other_vals)
    out = jnp.dot(attended, w_out.reshape(channels, channels), preferred_element_type=jnp.float32)
    return (half.astype(jnp.float32) + out.reshape(half.shape)).astype(jnp.bfloat16)


def solution(mesh):
    lat_spec = P("dp", "sp", "sp2", None)

    def local(x, time_emb, gn_scale, gn_shift, conv_w, time_w, w_qkv, w_out):
        _, core = place(lax.axis_index(SP))
        norms = gn_scale, gn_shift
        hidden, half, sums, edge, time_vec = conv_in(x, gn_scale, gn_shift, time_emb, time_w, conv_w)
        first, sums, _ = conv(hidden, swap_cores(edge), sums, swap_cores(sums), *norms, 1, conv_w, 1, half)
        middle = attention_block(first, sums, gn_scale[2], gn_shift[2], w_qkv, w_out)
        sums, edge = channel_sums(middle), edge_of(middle, core)
        hidden, sums, edge = conv(middle, swap_cores(edge), sums, swap_cores(sums), *norms, 3, conv_w, 2, time_vec)
        return conv_out(hidden, swap_cores(edge), sums, swap_cores(sums), *norms, 4, conv_w, 3, middle)

    return jax.shard_map(local, mesh=mesh, in_specs=(lat_spec, P("dp", None), P(), P(), P(), P(), P(), P()), out_specs=lat_spec, check_vma=False)
```
